32 devices in a mesh: row: 4 (over y, core), col: 8 (over z, x).
Axes of the slice: x: 2, y: 2, z: 4, core: 2. Of those that a mesh axis runs over, the one named last changes fastest.
Arguments:
- obs_cell: int32 [32, 16, 32, 128], P(('row', 'col')), may hold values from 0 to 8388607, as said below
- obs_value: bfloat16 [32, 16, 32, 128], P(('row', 'col')), may hold values from -6 to 6
- obs_weight: bfloat16 [32, 16, 32, 128], P(('row', 'col')), may hold values from 0.5 to 2
- obs_count: int32 [32, 16, 32], P(('row', 'col')), may hold values from 0 to 128, as said below
- kappa_field: float32 [2048, 4096], P('row', 'col'), may hold values from 0.2 to 6
Outputs:
- solution_field: float32 [2048, 4096], P('row', 'col')
- residual: float32 [2048, 4096], P('row', 'col')
The draws below stay inside these ranges and needn't reach their ends.
Inputs may be any that keep to these rules, and one draw needn't show every extreme that they name: `obs_cell`: block (s, t, d) holds observations for tile t of device d, where device d is number d // 8 along row and d % (8) along col, and tile t is number t // 4 among the device's tiles along rows and t % (4) along columns, each tile 128 by 128 cells; every slot of the block, padding included, names a cell of that tile as row * 4096 + column. Slots at positions obs_count and beyond are padding. For one owner device, chosen afresh in each draw, every block from every source and tile is full.
All inputs are finite; a program needn't handle non-finite values.
Results may differ from the reference program's by a relative error of at most 0.0029.
Values may be sent and summed in bfloat16 or wider, within the bound.
A program may use at most 64 MiB of HBM per device.

```python
import math
import jax
import jax.numpy as jnp
from jax import lax

CR = 512
CC = 512
TILE = 128
BLOCK = 128
ITERS = 3
TILES = 16
NR = 2048
NC = 4096
DEVICES = 32


def draw_obs_count(key, part):
    key_pop, key_hot, key_load = jax.random.split(jax.random.fold_in(key, 11), 3)
    owners = jnp.arange(DEVICES, dtype=jnp.int32)
    popular = jax.random.randint(key_pop, (DEVICES,), 1, 5, dtype=jnp.int32)
    hottest = jax.random.randint(key_hot, (), 0, DEVICES, dtype=jnp.int32)
    popular = jnp.where(owners == hottest, 8, popular)
    raw_load = jax.random.randint(key_load, (DEVICES, TILES, DEVICES), 0, 2 * BLOCK + 1, dtype=jnp.int32)
    counts = jnp.minimum(BLOCK, raw_load * popular[None, None, :] // 4)
    counts = jnp.where(owners[None, None, :] == hottest, BLOCK, counts)
    return counts.astype(jnp.int32)


def draw_obs_cell(key, part):
    key_row, key_col = jax.random.split(jax.random.fold_in(key, 23))
    full_shape = (DEVICES, TILES, DEVICES, BLOCK)
    local_row = jax.random.randint(key_row, full_shape, 0, TILE, dtype=jnp.int32)
    local_col = jax.random.randint(key_col, full_shape, 0, TILE, dtype=jnp.int32)
    owners = jnp.arange(DEVICES, dtype=jnp.int32)[None, None, :, None]
    tile_ids = jnp.arange(TILES, dtype=jnp.int32)[None, :, None, None]
    grid_cols = NC // CC
    tile_span = CC // TILE
    lattice_row = owners // grid_cols * CR + tile_ids // tile_span * TILE + local_row
    lattice_col = owners % grid_cols * CC + tile_ids % tile_span * TILE + local_col
    return (lattice_row * NC + lattice_col).astype(jnp.int32)


def steps_of(own_key, extent, pieces, smallest, largest):
    def one(axis_at, shards_of):
        steps = jax.random.uniform(jax.random.fold_in(jax.random.fold_in(own_key, 6), axis_at), (shards_of,), jnp.float32, smallest / len(pieces), largest / len(pieces))
        return jnp.repeat(jnp.exp(steps), extent[axis_at] // shards_of).reshape((-1,) + (1,) * (len(extent) - axis_at - 1))

    gain = one(*pieces[0])
    for cut in pieces[1:]:
        gain = gain * one(*cut)
    return gain


def normal_values(key, extent, width, limit, cuts=(), held_as=jnp.bfloat16):
    array = jax.random.normal(key, extent, jnp.float32) * width
    if len(cuts) > 0:
        array = steps_of(key, extent, cuts, -0.22, 0.18) * array
    return jnp.clip(array, min=-limit, max=limit).astype(held_as)


def setup_inputs(seed: int = 0) -> dict:
    key_of = jax.random.split(jax.random.key(seed), 6)
    obs_cell = draw_obs_cell(jax.random.fold_in(key_of[5], 71), 0)
    obs_value = normal_values(key_of[1], (DEVICES, TILES, DEVICES, BLOCK), 1.0, 6.0, ((0, 32),))
    obs_weight = jnp.clip(jnp.exp(math.log(2.0) - 1.3862944 * jax.random.uniform(key_of[2], (DEVICES, TILES, DEVICES, BLOCK), jnp.float32) ** steps_of(key_of[2], (DEVICES, TILES, DEVICES, BLOCK), ((0, 32),), -0.2, 0.2)), 0.5, 2.0).astype(jnp.bfloat16)
    obs_count = draw_obs_count(jax.random.fold_in(key_of[5], 71), 0)
    kappa_field = jnp.clip(jnp.exp(math.log(6.0) - 3.4011974 * jax.random.uniform(key_of[4], (NR, NC), jnp.float32) ** steps_of(key_of[4], (NR, NC), ((0, 4), (1, 8)), -0.2, 0.2)), 0.2, 6.0)
    return {"obs_cell": obs_cell, "obs_value": obs_value, "obs_weight": obs_weight, "obs_count": obs_count, "kappa_field": kappa_field}


smooth_weight = 0.05


def stencil_step(field, kappa_field):
    padded = jnp.pad(field, 1)
    beside = padded[2:, 1:-1] + padded[:-2, 1:-1]
    beside = beside + padded[1:-1, 2:] + padded[1:-1, :-2]
    return (4.0 + kappa_field) * field - beside


def reference(obs_cell, obs_value, obs_weight, obs_count, kappa_field):
    rows_all, cols_all = kappa_field.shape
    positions = jnp.arange(BLOCK, dtype=jnp.int32)
    is_live = positions < obs_count[..., None]
    weight_wide = obs_weight.astype(jnp.float32)
    product = (weight_wide * obs_value.astype(jnp.float32)).astype(jnp.bfloat16)
    product = lax.optimization_barrier(product)
    masked_weight = jnp.where(is_live, weight_wide, jnp.float32(0.0)).reshape(-1)
    masked_resp = jnp.where(is_live, product.astype(jnp.float32), jnp.float32(0.0)).reshape(-1)
    flat_cells = obs_cell.reshape(-1).astype(jnp.int32)
    empty = jnp.zeros((rows_all * cols_all,), jnp.float32)
    weight_field = empty.at[flat_cells].add(masked_weight).reshape(rows_all, cols_all)
    response = empty.at[flat_cells].add(masked_resp).reshape(rows_all, cols_all)

    def operate(field):
        inner = stencil_step(field, kappa_field)
        return weight_field * field + smooth_weight * stencil_step(inner, kappa_field)

    solution_field = jnp.zeros_like(response)
    residual, direction = response, response
    norm_now = jnp.sum(residual * residual)
    for step in range(ITERS):
        image = operate(direction)
        alpha = norm_now / jnp.sum(direction * image)
        solution_field = solution_field + alpha * direction
        residual = residual - alpha * image
        norm_next = jnp.sum(residual * residual)
        direction = residual + (norm_next / norm_now) * direction
        norm_now = norm_next
    return solution_field, residual
```

```python
import functools

import jax
import jax.numpy as jnp
from jax import lax
from jax.experimental import pallas as pl
from jax.experimental.pallas import tpu as pltpu
from jax.sharding import PartitionSpec as P

TILE = 128
ITERS = 3
HALO = 8
PAD = 2 * HALO
STRIP = 176
GROUP = 8
LANES = 128
MARGIN = 16
BAND = 16
LIMIT = 2000.0

smooth_weight = 0.05

MESH = pl.DeviceIdType.MESH


def greet_all(me, count, cols):
    barrier = pltpu.get_barrier_semaphore()

    def signal(k, carry):
        peer = lax.rem(me + k, count)
        pl.semaphore_signal(
            barrier, inc=1, device_id=(peer // cols, lax.rem(peer, cols)), device_id_type=MESH
        )
        return carry

    lax.fori_loop(1, count, signal, 0)


def await_all(count):
    pl.semaphore_wait(pltpu.get_barrier_semaphore(), count - 1)


def smooth_kernel(
    rows, cols, b_ref, w_ref, k_ref, x_ref, r_ref,
    res, wgt, kap, live, inner, image, along, second, further, course,
    send_low, send_high, recv_low, recv_high, mine, sums,
    row_send, row_recv, col_send, col_recv, sum_send, sum_recv,
):
    count = rows * cols
    my_row, my_col = lax.axis_index("row"), lax.axis_index("col")
    me = my_row * cols + my_col
    height, width = b_ref.shape
    full = width + 128
    own = pl.ds(PAD, height)
    fields = ((b_ref, res), (w_ref, wgt), (k_ref, kap))
    tall = res.shape[0]

    for _, field in fields:
        field[0:PAD, :] = jnp.zeros((PAD, full), jnp.float32)
        field[PAD + height :, :] = jnp.zeros((tall - PAD - height, full), jnp.float32)
    inner[0:HALO, :] = jnp.zeros((HALO, full), jnp.float32)
    inner[PAD + height + HALO : 2 * PAD + height, :] = jnp.zeros((HALO, full), jnp.float32)
    recv_low[...] = jnp.zeros_like(recv_low)
    recv_high[...] = jnp.zeros_like(recv_high)
    greet_all(me, count, cols)

    def fill(i, carry):
        at = pl.multiple_of(i * 32, 32)
        for src, dst in fields:
            dst[pl.ds(PAD + at, 32), 0:width] = src[pl.ds(at, 32), :]
        return carry

    lax.fori_loop(0, height // 32, fill, 0)

    await_all(count)

    up, down = my_row > 0, my_row < rows - 1
    left, right = my_col > 0, my_col < cols - 1

    def row_copies(way):
        made = []
        for at, (src, dst) in enumerate(fields):
            if way == 0:
                source, target = src.at[pl.ds(0, HALO), :], dst.at[pl.ds(PAD + height, HALO), pl.ds(0, width)]
                where = (my_row - 1, my_col)
            else:
                source, target = src.at[pl.ds(height - HALO, HALO), :], dst.at[pl.ds(HALO, HALO), pl.ds(0, width)]
                where = (my_row + 1, my_col)
            made.append(
                pltpu.make_async_remote_copy(
                    src_ref=source, dst_ref=target,
                    send_sem=row_send.at[way, at], recv_sem=row_recv.at[way, at],
                    device_id=where, device_id_type=MESH,
                )
            )
        return made

    def col_copy(way):
        source, target, where = (
            (send_low, recv_high, (my_row, my_col - 1)),
            (send_high, recv_low, (my_row, my_col + 1)),
        )[way]
        return pltpu.make_async_remote_copy(
            src_ref=source, dst_ref=target, send_sem=col_send.at[way], recv_sem=col_recv.at[way],
            device_id=where, device_id_type=MESH,
        )

    for way, there in ((0, up), (1, down)):

        @pl.when(there)
        def _(way=way):
            for copy in row_copies(way):
                copy.start()

    for way, there in ((0, up), (1, down)):

        @pl.when(there)
        def _(way=way):
            for copy in row_copies(way):
                copy.wait_send()

        @pl.when((down, up)[way])
        def _(way=way):
            for copy in row_copies(way):
                copy.wait_recv()

    def pack(i, carry):
        at = pl.multiple_of(i * 128, 128)
        for which, (_, field) in enumerate(fields):
            low = field[pl.ds(at, 128), 0:128].T
            send_low[which * HALO : (which + 1) * HALO, pl.ds(at, 128)] = low[:HALO]
            high = field[pl.ds(at, 128), width - 128 : width].T
            send_high[which * HALO : (which + 1) * HALO, pl.ds(at, 128)] = high[128 - HALO :]
        return carry

    lax.fori_loop(0, tall // 128, pack, 0, unroll=True)
    for way, there in ((0, left), (1, right)):

        @pl.when(there)
        def _(way=way):
            col_copy(way).start()

    for way, there in ((0, left), (1, right)):

        @pl.when(there)
        def _(way=way):
            col_copy(way).wait_send()

        @pl.when((right, left)[way])
        def _(way=way):
            col_copy(way).wait_recv()

    gap = jnp.zeros((128 - 2 * HALO, 128), jnp.float32)

    def unpack(i, carry):
        at = pl.multiple_of(i * 128, 128)
        for which, (_, field) in enumerate(fields):
            part = slice(which * HALO, (which + 1) * HALO)
            both = jnp.concatenate(
                [recv_high[part, pl.ds(at, 128)], gap, recv_low[part, pl.ds(at, 128)]], axis=0
            )
            field[pl.ds(at, 128), width:full] = both.T
        return carry

    lax.fori_loop(0, tall // 128, unpack, 0, unroll=True)

    strips = (height + 2 * HALO) // STRIP
    top = jnp.where(up, HALO, PAD)
    bottom = PAD + height + jnp.where(down, HALO, 0)
    high_end = width + jnp.where(right, HALO, 0)
    low_begin = full - jnp.where(left, HALO, 0)

    def start_of(i):
        return pl.multiple_of(HALO + i * STRIP, 8)

    def prepare(i, carry):
        at = start_of(i)
        row = lax.broadcasted_iota(jnp.int32, (STRIP, full), 0) + at
        col = lax.broadcasted_iota(jnp.int32, (STRIP, full), 1)
        inside = (row >= top) & (row < bottom) & ((col < high_end) | (col >= low_begin))
        mask = jnp.where(inside, 1.0, 0.0).astype(jnp.float32)
        live[pl.ds(at, STRIP), :] = mask
        kap[pl.ds(at, STRIP), :] = jnp.where(inside, 4.0 + kap[pl.ds(at, STRIP), :], 0.0)
        return carry

    lax.fori_loop(0, strips, prepare, 0)

    def stencil(field, at):
        slab = field[pl.ds(pl.multiple_of(at - HALO, 8), STRIP + 2 * HALO), :]
        center = slab[HALO : HALO + STRIP]
        beside = slab[HALO + 1 : HALO + 1 + STRIP] + slab[HALO - 1 : HALO - 1 + STRIP]
        beside = beside + pltpu.roll(center, full - 1, axis=1) + pltpu.roll(center, 1, axis=1)
        here = pl.ds(at, STRIP)
        return kap[here, :] * center - live[here, :] * beside

    def operate(source, target):
        def first(i, carry):
            at = start_of(i)
            inner[pl.ds(at, STRIP), :] = stencil(source, at)
            return carry

        def last(i, carry):
            at = start_of(i)
            here = pl.ds(at, STRIP)
            target[here, :] = wgt[here, :] * source[here, :] + smooth_weight * stencil(inner, at)
            return carry

        lax.fori_loop(0, strips, first, 0)
        lax.fori_loop(0, strips, last, 0)

    lane = lax.broadcasted_iota(jnp.int32, (1, 128), 1)

    def copy_to(step, k, peer, slot):
        return pltpu.make_async_remote_copy(
            src_ref=mine.at[step], dst_ref=sums.at[step, slot],
            send_sem=sum_send.at[step, k], recv_sem=sum_recv.at[step, k],
            device_id=(peer // cols, lax.rem(peer, cols)), device_id_type=MESH,
        )

    def begin_products(step):
        def add(i, carry):
            norm, curve = carry
            here = pl.ds(pl.multiple_of(PAD + i * 32, 8), 32)
            a, c = res[here, 0:width], image[here, 0:width]
            aa, ac = a * a, a * c
            norm = norm + ((aa[:8] + aa[8:16]) + (aa[16:24] + aa[24:]))
            return norm, curve + ((ac[:8] + ac[8:16]) + (ac[16:24] + ac[24:]))

        zero = jnp.zeros((8, width), jnp.float32)
        norm, curve = lax.fori_loop(0, height // 32, add, (zero, zero))
        norm = jnp.sum(jnp.sum(norm, axis=0, keepdims=True), axis=1, keepdims=True)
        curve = jnp.sum(jnp.sum(curve, axis=0, keepdims=True), axis=1, keepdims=True)
        both = jnp.where(lane == 0, norm, jnp.where(lane == 1, curve, 0.0))
        mine[step] = both
        sums[step, me] = both

        def begin(k, carry):
            copy_to(step, k, lax.rem(me + k, count), me).start()
            return carry

        lax.fori_loop(1, count, begin, 0, unroll=True)

    def end_products(step):
        def finish(k, carry):
            source = lax.rem(me + count - k, count)
            copy_to(step, k, source, source).wait()
            return carry

        lax.fori_loop(1, count, finish, 0, unroll=True)
        total = jnp.sum(sums[step], axis=0)
        norm = jnp.sum(jnp.where(lane == 0, total, 0.0), axis=1, keepdims=True)
        curve = jnp.sum(jnp.where(lane == 1, total, 0.0), axis=1, keepdims=True)
        return norm, curve

    operate(res, image)
    begin_products(0)
    norm_now = alpha = None
    for step in range(ITERS):
        if step + 1 < ITERS:
            operate(image, second)
        norm_next, curvature = end_products(step)
        if step == 0:
            ratio = None
            alpha = norm_next / curvature
        else:
            ratio = norm_next / norm_now
            alpha = norm_next / (curvature - ratio * norm_next / alpha)
        norm_now = norm_next

        if step + 1 < ITERS:

            def recede(i, carry, step=step, ratio=ratio, alpha=alpha):
                here = pl.ds(pl.multiple_of(HALO + i * 48, 8), 48)
                way, path, next_path = res[here, :], image[here, :], second[here, :]
                old, old_image = way, path
                if step > 0:
                    way = way + ratio * course[here, :]
                    path = path + ratio * along[here, :]
                    next_path = next_path + ratio * further[here, :]
                course[here, :] = way
                along[here, :] = path
                further[here, :] = next_path
                res[here, :] = old - alpha * path
                image[here, :] = old_image - alpha * next_path
                return carry

            lax.fori_loop(0, (height + 2 * HALO) // 48, recede, 0)
            begin_products(step + 1)

        def advance(i, carry, step=step, ratio=ratio, alpha=alpha):
            at = pl.multiple_of(i * 32, 32)
            here = pl.ds(pl.multiple_of(PAD + at, 8), 32)
            rows_here = pl.ds(at, 32)
            if step + 1 < ITERS:
                moved = alpha * course[here, 0:width]
            else:
                moved = alpha * (res[here, 0:width] + ratio * course[here, 0:width])
                r_ref[rows_here, :] = res[here, 0:width] - alpha * (
                    image[here, 0:width] + ratio * along[here, 0:width]
                )
            x_ref[rows_here, :] = moved if step == 0 else x_ref[rows_here, :] + moved
            return carry

        lax.fori_loop(0, height // 32, advance, 0)


def edge_and_inner(down, across):
    edge = 2 * across + 2 * (down - 2)
    return edge, (down - 2) * (across - 2)


def edge_tile(e, down, across):
    side = e - across
    last = across + 2 * (down - 2)
    row = jnp.where(e < across, 0, jnp.where(e < last, 1 + side // 2, down - 1))
    col = jnp.where(e < across, e, jnp.where(e < last, lax.rem(side, 2) * (across - 1), e - last))
    return row, col


def inner_tile(e, down, across):
    return 1 + e // (across - 2), 1 + lax.rem(e, across - 2)


def split(value, size):
    if size & (size - 1) == 0:
        return lax.shift_right_logical(value, size.bit_length() - 1), value & (size - 1)
    return lax.div(value, size), lax.rem(value, size)


def flip(place, code, size):
    total, unit = 0, 1
    while unit < size:
        total = total + unit * lax.rem(place // unit + code // unit, 2)
        unit *= 2
    return total


def field_kernel(
    rows, cols, cell_hbm, value_hbm, weight_hbm, count_ref, kappa_hbm,
    bw, first, second, third, coef, good,
    cell_in, value_in, weight_in, cell_wide, value_wide, weight_wide,
    code_out, pair_out, code_out_inner, pair_out_inner,
    code_in, pair_in, code_in_inner, pair_in_inner,
    place_row, place_col, amounts, kap, mid,
    low_out, high_out, low_in, high_in, kap_low_out, kap_high_out, kap_low_in, kap_high_in,
    mine, sums,
    load_sems, send_sem, recv_sems, halo_send, halo_recv, sum_send, sum_recv,
):
    count = rows * cols
    my_row, my_col = lax.axis_index("row"), lax.axis_index("col")
    me = my_row * cols + my_col
    height, width = kappa_hbm.shape
    down, across = height // TILE, width // TILE
    tiles = down * across
    slots = code_in.shape[2]
    edges, inners = edge_and_inner(down, across)
    pitch = cell_wide.shape[0] // tiles
    bottom = MARGIN + height
    lane = lax.broadcasted_iota(jnp.int32, (1, LANES), 1)

    loads = [
        pltpu.make_async_copy(cell_hbm, cell_in, load_sems.at[0]),
        pltpu.make_async_copy(value_hbm, value_in, load_sems.at[1]),
        pltpu.make_async_copy(weight_hbm, weight_in, load_sems.at[2]),
    ]
    kappa_loads = [
        pltpu.make_async_copy(
            kappa_hbm.at[:, pl.ds(c * LANES, LANES)], kap.at[c, pl.ds(MARGIN, height), :], load_sems.at[3 + c]
        )
        for c in range(across)
    ]
    for load in loads + kappa_loads:
        load.start()

    for ref in (low_in, high_in, kap_low_in, kap_high_in):
        ref[...] = jnp.zeros_like(ref)
    strip = jnp.zeros((MARGIN, LANES), jnp.float32)
    for c in range(across):
        for field in (bw.at[0], bw.at[1], kap):
            field[c, 0:MARGIN, :] = strip
            field[c, bottom : bottom + MARGIN, :] = strip
    greet_all(me, count, cols)

    for field in (bw.at[0], bw.at[1], kap):
        field[across, 0:MARGIN, :] = strip
        field[across, bottom : bottom + MARGIN, :] = strip
    for c in range(across + 1):
        for field in (mid, first, second):
            field[c, 0:8, :] = strip[:8]
            field[c, bottom + 8 : bottom + 16, :] = strip[:8]

    def person(k):
        code_col, code_row = k // rows, lax.rem(k, rows)
        return flip(my_row, code_row, rows), flip(my_col, code_col, cols)

    for load in loads:
        load.wait()

    def widen(t, carry):
        here = pl.ds(pl.multiple_of(t * count, 8), count)
        there = pl.ds(pl.multiple_of(t * pitch, 8), count)
        cell_wide[there, :] = cell_in[here, :]
        weight = weight_in[here, :].astype(jnp.float32)
        weight_wide[there, :] = weight
        value_wide[there, :] = weight * value_in[here, :].astype(jnp.float32)
        return carry

    lax.fori_loop(0, tiles, widen, 0)
    dest_lane = lax.broadcasted_iota(jnp.int32, count_ref.shape, 1)
    slot_lane = lax.broadcasted_iota(jnp.int32, (tiles, slots), 1).astype(jnp.float32)
    edge_ids = [t for t in range(tiles) if t // across in (0, down - 1) or t % across in (0, across - 1)]
    inner_ids = [t for t in range(tiles) if t not in edge_ids]

    def pick(value, ids):
        parts, begin = [], 0
        while begin < len(ids):
            end = begin
            while end + 1 < len(ids) and ids[end + 1] == ids[end] + 1:
                end += 1
            parts.append(value[ids[begin] : ids[end] + 1])
            begin = end + 1
        return jnp.concatenate(parts, axis=0) if len(parts) > 1 else parts[0]

    def encode(k, carry):
        row, col = person(k)
        dest = row * cols + col
        every = pl.ds(dest, tiles, stride=pitch)
        cell = cell_wide[every, :]
        upper, _ = split(cell, width * cols)
        local = split(upper, TILE)[1] * TILE + split(cell, TILE)[1]
        alive = jnp.sum(jnp.where(dest_lane == dest, count_ref[...], 0.0), axis=1, keepdims=True)
        local = jnp.where(slot_lane < alive, local, -1)
        weight, product = weight_wide[every, :], value_wide[every, :]
        code_out[k] = pick(local, edge_ids).astype(jnp.int16)
        pair_out[k] = jnp.concatenate([pick(weight, edge_ids), pick(product, edge_ids)], axis=0).astype(jnp.bfloat16)
        code_out_inner[k] = pick(local, inner_ids).astype(jnp.int16)
        pair_out_inner[k] = jnp.concatenate(
            [pick(weight, inner_ids), pick(product, inner_ids)], axis=0
        ).astype(jnp.bfloat16)
        return carry

    lax.fori_loop(0, count, encode, 0, unroll=2)
    pieces = (
        ((code_out, code_in), (pair_out, pair_in), edges, edge_tile),
        ((code_out_inner, code_in_inner), (pair_out_inner, pair_in_inner), inners, inner_tile),
    )
    for piece in pieces:
        for source, target in piece[:2]:
            target[0] = source[0]
    await_all(count)

    bunch = GROUP
    chunks = count // bunch

    def send(piece, begin, end):
        def one(k, carry):
            place = person(k)
            for which, (source, target) in enumerate(pieces[piece][:2]):
                pltpu.make_async_remote_copy(
                    src_ref=source.at[k], dst_ref=target.at[k],
                    send_sem=send_sem.at[piece, which], recv_sem=recv_sems.at[k // bunch, piece, which],
                    device_id=place, device_id_type=MESH,
                ).start()
            return carry

        lax.fori_loop(begin, end, one, 0)

    half = count // 2
    send(0, half, count)
    send(0, 1, half)
    send(1, 1, half)
    send(1, half, count)

    def halo_copies(group, body, parts):
        low_from, high_from, low_to, high_to = parts
        up_rows, down_rows = pl.ds(MARGIN, 8), pl.ds(bottom - 8, 8)
        above, below = pl.ds(MARGIN - 8, 8), pl.ds(bottom, 8)
        main = pl.ds(LANES, height)
        head, tail = pl.ds(0, LANES), pl.ds(LANES + height, LANES)
        begin, end = pl.ds(0, LANES), pl.ds(height - LANES, LANES)
        whole = pl.ds(0, height)
        plan = [
            (-1, 0, body(up_rows), body(below)),
            (1, 0, body(down_rows), body(above)),
            (0, -1, low_from.at[:, whole], high_to.at[:, main]),
            (0, 1, high_from.at[:, whole], low_to.at[:, main]),
            (-1, -1, low_from.at[:, begin], high_to.at[:, tail]),
            (1, -1, low_from.at[:, end], high_to.at[:, head]),
            (-1, 1, high_from.at[:, begin], low_to.at[:, tail]),
            (1, 1, high_from.at[:, end], low_to.at[:, head]),
        ]
        made = []
        for at, (dr, dc, source, target) in enumerate(plan):

            def there(dr=dr, dc=dc):
                ok = True
                for step, place, size in ((dr, my_row, rows), (dc, my_col, cols)):
                    if step < 0:
                        ok = (place > 0) & ok
                    if step > 0:
                        ok = (place < size - 1) & ok
                return ok

            copy = pltpu.make_async_remote_copy(
                src_ref=source, dst_ref=target,
                send_sem=halo_send.at[group, at], recv_sem=halo_recv.at[group, at],
                device_id=(my_row + dr, my_col + dc), device_id_type=MESH,
            )
            made.append((there(), there(-dr, -dc), copy))
        return made

    def start_halo(copies):
        for goes, _, copy in copies:

            @pl.when(goes)
            def _(copy=copy):
                copy.start()

    def end_halo(copies):
        for goes, comes, copy in copies:

            @pl.when(goes)
            def _(copy=copy):
                copy.wait_send()

            @pl.when(comes)
            def _(copy=copy):
                copy.wait_recv()

    def pack(field, at, low, high):
        for j in range(down):
            here = pl.ds(MARGIN + j * TILE, TILE)
            there = slice(j * TILE, (j + 1) * TILE)
            low[at : at + 8, there] = field[0, here, :].T[:8]
            high[at : at + 8, there] = field[across - 1, here, :].T[TILE - 8 :]

    gap = jnp.zeros((LANES - 16, LANES), jnp.float32)

    def unpack(field, at, low, high):
        for j in range(-1, down + 1):
            lanes = slice(LANES + j * TILE, LANES + (j + 1) * TILE)
            both = jnp.concatenate([high[at : at + 8, lanes], gap, low[at : at + 8, lanes]], axis=0).T
            if j < 0:
                field[across, MARGIN - 8 : MARGIN, :] = both[TILE - 8 :]
            elif j == down:
                field[across, bottom : bottom + 8, :] = both[:8]
            else:
                field[across, MARGIN + j * TILE : MARGIN + (j + 1) * TILE, :] = both

    kap_halo = halo_copies(
        0, lambda part: kap.at[pl.ds(0, across), part, :], (kap_low_out, kap_high_out, kap_low_in, kap_high_in)
    )
    bw_halo = halo_copies(
        1, lambda part: bw.at[:, pl.ds(0, across), part, :], (low_out, high_out, low_in, high_in)
    )
    for load in kappa_loads:
        load.wait()
    pack(kap, 0, kap_low_out, kap_high_out)
    start_halo(kap_halo)

    offsets = lax.broadcasted_iota(jnp.int32, (TILE, slots), 0).astype(jnp.float32).astype(jnp.bfloat16)
    one = jnp.ones((TILE, slots), jnp.bfloat16)
    zero = jnp.zeros((TILE, slots), jnp.bfloat16)

    def bin_chunk(chunk, piece):
        codes, pairs, some, locate = pieces[piece]
        for which, (_, target) in enumerate((codes, pairs)):
            begin = chunk * bunch + (1 if chunk == 0 else 0)
            part = target.at[pl.ds(begin, (chunk + 1) * bunch - begin)]
            pltpu.make_async_copy(part, part, recv_sems.at[chunk, piece, which]).wait()
        for n in range(bunch):
            code = codes[1][chunk * bunch + n].astype(jnp.int32)
            place_row[n * some : (n + 1) * some, :] = (code >> 7).astype(jnp.float32)
            place_col[n * some : (n + 1) * some, :] = (code & (TILE - 1)).astype(jnp.float32)
            amounts[n * 2 * some : (n + 1) * 2 * some, :] = pairs[1][chunk * bunch + n].astype(jnp.float32)

        def spread(ref, at):
            return jnp.broadcast_to(ref[pl.ds(at, 1), :].astype(jnp.bfloat16), (TILE, slots))

        def bin_tile(e, carry):
            hot, weights, products = [], [], []
            for n in range(bunch):
                hot.append(jnp.where(spread(place_col, n * some + e) == offsets, one, zero))
                hit = spread(place_row, n * some + e) == offsets
                weights.append(jnp.where(hit, spread(amounts, n * 2 * some + e), zero))
                products.append(jnp.where(hit, spread(amounts, n * 2 * some + some + e), zero))
            stacked = jnp.concatenate(
                [jnp.concatenate(products, axis=1), jnp.concatenate(weights, axis=1)], axis=0
            )
            total = lax.dot_general(
                stacked, jnp.concatenate(hot, axis=1), (((1,), (1,)), ((), ())),
                preferred_element_type=jnp.float32,
            )
            row, col = locate(e, down, across)
            here = pl.ds(pl.multiple_of(MARGIN + row * TILE, 8), TILE)
            if chunk == 0:
                bw[0, col, here, :] = total[:TILE]
                bw[1, col, here, :] = total[TILE:]
            else:
                bw[0, col, here, :] += total[:TILE]
                bw[1, col, here, :] += total[TILE:]
            return carry

        lax.fori_loop(0, some, bin_tile, 0, unroll=4)

    for chunk in range(chunks // 2):
        bin_chunk(chunk, 0)
        bin_chunk(chunk, 1)
    for chunk in range(chunks // 2, chunks):
        bin_chunk(chunk, 0)
    for which in range(2):
        pack(bw.at[which], 8 * which, low_out, high_out)
    start_halo(bw_halo)
    for chunk in range(chunks // 2, chunks):
        bin_chunk(chunk, 1)
    end_halo(kap_halo)
    unpack(kap, 0, kap_low_in, kap_high_in)
    for piece in range(2):
        for which, (source, _) in enumerate(pieces[piece][:2]):
            part = source.at[pl.ds(1, count - 1)]
            pltpu.make_async_copy(part, part, send_sem.at[piece, which]).wait()
    end_halo(bw_halo)
    for which in range(2):
        unpack(bw.at[which], 8 * which, low_in, high_in)

    up, under = my_row > 0, my_row < rows - 1
    live = ((lane < 8) & (my_col < cols - 1)) | ((lane >= LANES - 8) & (my_col > 0))

    def inner(field, at, size, columns):
        every = range(across + 1)
        here = pl.ds(at, size)
        center = [field[c, here, :] for c in every]
        ahead = [pltpu.roll(x, 1, axis=1) for x in center]
        behind = [pltpu.roll(x, LANES - 1, axis=1) for x in center]
        result = []
        for c in range(columns):
            beside = field[c, pl.ds(at - 1, size), :] + field[c, pl.ds(at + 1, size), :]
            beside = beside + jnp.where(lane == 0, ahead[c - 1], ahead[c])
            beside = beside + jnp.where(lane == LANES - 1, behind[(c + 1) % (across + 1)], behind[c])
            value = (4.0 + kap[c, here, :]) * center[c] - beside
            result.append(jnp.where(live, value, 0.0) if c == across else value)
        return result

    response, weight = bw.at[0], bw.at[1]
    outer = ((MARGIN - 8, up), (bottom, under))

    def bands(body, carry):
        def step(i, carry):
            return body(pl.multiple_of(MARGIN + i * BAND, 8), carry)

        return lax.fori_loop(0, height // BAND, step, carry)

    def fold(value):
        total = value[0:8]
        for n in range(8, value.shape[0], 8):
            total = total + value[n : n + 8]
        return total

    def apply_inner(source):
        def body(at, carry):
            square, energy = carry
            for c, value in enumerate(inner(source, at, BAND, across + 1)):
                here = pl.ds(at, BAND)
                mid[c, here, :] = value
                if c < across:
                    x = source[c, here, :]
                    xx = x * x
                    square = square + fold(xx)
                    energy = energy + fold(weight[c, here, :] * xx + smooth_weight * (value * value))
            return square, energy

        blank = jnp.zeros((8, LANES), jnp.float32)
        result = bands(body, (blank, blank))
        for at, there in outer:
            for c, value in enumerate(inner(source, at, 8, across + 1)):
                mid[c, pl.ds(at, 8), :] = jnp.where(there, value, 0.0)
        return result

    def apply_outer(source, target):
        def store(at, size, there=None):
            for c, value in enumerate(inner(mid, at, size, across + 1)):
                here = pl.ds(at, size)
                value = weight[c, here, :] * source[c, here, :] + smooth_weight * value
                target[c, here, :] = value if there is None else jnp.where(there, value, 0.0)

        def body(at, carry):
            store(at, BAND)
            return carry

        bands(body, 0)
        for at, there in outer:
            store(at, 8, there)

    moments = []
    moments += apply_inner(response)
    apply_outer(response, first)
    moments += apply_inner(first)
    apply_outer(first, second)
    moments += apply_inner(second)

    both = jnp.zeros((1, LANES), jnp.float32)
    for at, value in enumerate(moments):
        total = jnp.sum(jnp.sum(value, axis=0, keepdims=True), axis=1, keepdims=True)
        both = jnp.where(lane == at, total, both)
    mine[...] = both
    sums[me] = both

    def sum_copy(k, slot):
        return pltpu.make_async_remote_copy(
            src_ref=mine, dst_ref=sums.at[slot],
            send_sem=sum_send.at[k], recv_sem=sum_recv.at[k],
            device_id=person(k), device_id_type=MESH,
        )

    def begin(i, carry):
        sum_copy(count - 1 - i, me).start()
        return carry

    lax.fori_loop(0, count - 1, begin, 0)

    def last(at, carry):
        for c, value in enumerate(inner(mid, at, BAND, across)):
            here = pl.ds(at, BAND)
            third[c, pl.ds(pl.multiple_of(at - MARGIN, 8), BAND), :] = (
                weight[c, here, :] * second[c, here, :] + smooth_weight * value
            )
        return carry

    bands(last, 0)

    def finish(k, carry):
        row, col = person(k)
        sum_copy(k, row * cols + col).wait()
        return carry

    lax.fori_loop(1, count, finish, 0)
    total = jnp.sum(sums[...], axis=0)
    m = [jnp.sum(jnp.where(lane == at, total, 0.0), axis=1, keepdims=True) for at in range(6)]
    scale = m[1] / m[0]
    power, n = scale, [None, None]
    for at in range(2, 6):
        power = power * scale
        n.append(m[at] / m[0] / power)
    fall = n[2] - 1.0
    bend = n[3] - n[2] * n[2]
    alpha = fall / bend
    a = 1.0 + alpha * n[2]
    lead = n[2] - a * n[3] + alpha * n[4]
    lead_size = n[2] + a * n[3] + alpha * n[4]
    beta = alpha * lead / fall
    d0, d1 = 1.0 + beta * n[2], a + beta
    turn = d0 * n[3] - d1 * n[4] + alpha * n[5]
    turn_size = d0 * n[3] + d1 * n[4] + alpha * n[5]
    step = lead / turn
    inverse = 1.0 / scale
    powers = [inverse, inverse * inverse, inverse * inverse * inverse]
    parts = [
        (1.0 + alpha * n[2] + step * d0) * powers[0],
        -(alpha + step * d1) * powers[1],
        step * alpha * powers[2],
        -(a + step * d0) * powers[0],
        (alpha + step * d1) * powers[1],
        -(step * alpha) * powers[2],
    ]
    for at, value in enumerate(parts):
        coef[at : at + 1, :] = jnp.broadcast_to(value, (1, LANES))
    coef[6:8, :] = jnp.zeros((2, LANES), jnp.float32)
    sound = (fall * LIMIT >= n[2]) & (bend * LIMIT >= n[3])
    sound = sound & (lead * LIMIT >= lead_size) & (turn * LIMIT >= turn_size)
    sound = sound & (alpha * lead * (2.0 * LIMIT) >= 1.0 + a * a * n[2] + alpha * alpha * n[4])
    good[...] = jnp.where(sound, 1, 0)


def combine_kernel(bw, first, second, third, coef, x_hbm, r_hbm, x_out, r_out, sems):
    across, height, _ = third.shape
    band = height // 8
    weights = [coef[at : at + 1, :] for at in range(6)]
    copies = []
    for i in range(8):
        rows_here = pl.ds(i * band, band)

        def body(j, carry, i=i):
            at = pl.multiple_of(i * band + j * 32, 8)
            for c in range(across):
                here = pl.ds(MARGIN + at, 32)
                values = [bw[0, c, here, :], first[c, here, :], second[c, here, :], third[c, pl.ds(at, 32), :]]
                lanes = slice(c * LANES, (c + 1) * LANES)
                x_out[pl.ds(at, 32), lanes] = (
                    weights[0] * values[0] + weights[1] * values[1] + weights[2] * values[2]
                )
                r_out[pl.ds(at, 32), lanes] = (
                    values[0] + weights[3] * values[1] + weights[4] * values[2] + weights[5] * values[3]
                )
            return carry

        lax.fori_loop(0, band // 32, body, 0)
        for at, (source, target) in enumerate(((x_out, x_hbm), (r_out, r_hbm))):
            copy = pltpu.make_async_copy(source.at[rows_here], target.at[rows_here], sems.at[i, at])
            copy.start()
            copies.append(copy)
    for copy in copies:
        copy.wait()


def per_device(rows, cols, obs_cell, obs_value, obs_weight, obs_count, kappa_field):
    count = rows * cols
    height, width = kappa_field.shape
    tiles, _, slots = obs_cell.shape[1:]
    down, across = height // TILE, width // TILE
    edges, inners = edge_and_inner(down, across)
    in_vmem = pl.BlockSpec(memory_space=pltpu.VMEM)
    anywhere = pl.BlockSpec(memory_space=pl.ANY)
    in_hbm = pl.BlockSpec(memory_space=pltpu.HBM)
    tall = height + 2 * MARGIN
    field = jax.ShapeDtypeStruct((height, width), jnp.float32)
    wide = jax.ShapeDtypeStruct((across + 1, tall, LANES), jnp.float32)
    pitch = count + 8
    flat = (tiles * count, slots)
    pitched = (tiles * pitch, slots)
    edge = [
        pltpu.VMEM((count, edges, slots), jnp.int16),
        pltpu.VMEM((count, 2 * edges, slots), jnp.bfloat16),
        pltpu.VMEM((count, inners, slots), jnp.int16),
        pltpu.VMEM((count, 2 * inners, slots), jnp.bfloat16),
    ]
    bw, first, second, third, coef, good = pl.pallas_call(
        functools.partial(field_kernel, rows, cols),
        out_shape=(
            jax.ShapeDtypeStruct((2, across + 1, tall, LANES), jnp.float32),
            wide,
            wide,
            jax.ShapeDtypeStruct((across, height, LANES), jnp.float32),
            jax.ShapeDtypeStruct((8, LANES), jnp.float32),
            jax.ShapeDtypeStruct((1, 1), jnp.int32),
        ),
        in_specs=[anywhere] * 3 + [in_vmem, anywhere],
        out_specs=(in_vmem,) * 6,
        scratch_shapes=[
            pltpu.VMEM(flat, jnp.int32),
            pltpu.VMEM(flat, jnp.bfloat16),
            pltpu.VMEM(flat, jnp.bfloat16),
            pltpu.VMEM(pitched, jnp.int32),
            pltpu.VMEM(pitched, jnp.float32),
            pltpu.VMEM(pitched, jnp.float32),
            *edge,
            *edge,
            pltpu.VMEM((GROUP * edges, slots), jnp.float32),
            pltpu.VMEM((GROUP * edges, slots), jnp.float32),
            pltpu.VMEM((GROUP * edges * 2, slots), jnp.float32),
            pltpu.VMEM(wide.shape, jnp.float32),
            pltpu.VMEM(wide.shape, jnp.float32),
            pltpu.VMEM((16, height), jnp.float32),
            pltpu.VMEM((16, height), jnp.float32),
            pltpu.VMEM((16, height + 2 * LANES), jnp.float32),
            pltpu.VMEM((16, height + 2 * LANES), jnp.float32),
            pltpu.VMEM((8, height), jnp.float32),
            pltpu.VMEM((8, height), jnp.float32),
            pltpu.VMEM((8, height + 2 * LANES), jnp.float32),
            pltpu.VMEM((8, height + 2 * LANES), jnp.float32),
            pltpu.VMEM((1, LANES), jnp.float32),
            pltpu.VMEM((count, 1, LANES), jnp.float32),
            pltpu.SemaphoreType.DMA((3 + across,)),
            pltpu.SemaphoreType.DMA((2, 2)),
            pltpu.SemaphoreType.DMA((count // GROUP, 2, 2)),
            pltpu.SemaphoreType.DMA((2, 8)),
            pltpu.SemaphoreType.DMA((2, 8)),
            pltpu.SemaphoreType.DMA((count,)),
            pltpu.SemaphoreType.DMA((count,)),
        ],
        compiler_params=pltpu.CompilerParams(
            collective_id=0, has_side_effects=True, vmem_limit_bytes=30 << 20
        ),
        name="fields",
    )(
        obs_cell.reshape(flat), obs_value.reshape(flat), obs_weight.reshape(flat),
        obs_count[0].astype(jnp.float32), kappa_field,
    )

    def combine(bw, first, second, third, coef, kappa):
        return pl.pallas_call(
            combine_kernel,
            out_shape=(field, field),
            in_specs=[in_vmem] * 5,
            out_specs=(in_hbm,) * 2,
            scratch_shapes=[
                pltpu.VMEM(field.shape, jnp.float32),
                pltpu.VMEM(field.shape, jnp.float32),
                pltpu.SemaphoreType.DMA((8, 2)),
            ],
            compiler_params=pltpu.CompilerParams(vmem_limit_bytes=16 << 20),
            name="combine",
        )(bw, first, second, third, coef)

    def iterate(bw, first, second, third, coef, kappa):
        own = bw[:, :across, MARGIN : MARGIN + height, :].transpose(0, 2, 1, 3).reshape(2, height, width)
        return smooth(rows, cols, own[0], own[1], kappa)

    return lax.cond(good[0, 0] > 0, combine, iterate, bw, first, second, third, coef, kappa_field)


def smooth(rows, cols, response, weight_field, kappa_field):
    count = rows * cols
    height, width = kappa_field.shape
    in_vmem = pl.BlockSpec(memory_space=pltpu.VMEM)
    field = jax.ShapeDtypeStruct((height, width), jnp.float32)
    full = width + 128
    tall = -(-(height + 2 * PAD) // 128) * 128
    extended = pltpu.VMEM((tall, full), jnp.float32)
    edge = pltpu.VMEM((3 * HALO, tall), jnp.float32)
    return pl.pallas_call(
        functools.partial(smooth_kernel, rows, cols),
        out_shape=(field, field),
        in_specs=[in_vmem] * 3,
        out_specs=(in_vmem,) * 2,
        scratch_shapes=[extended] * 10
        + [edge] * 4
        + [
            pltpu.VMEM((ITERS, 1, 128), jnp.float32),
            pltpu.VMEM((ITERS, count, 1, 128), jnp.float32),
            pltpu.SemaphoreType.DMA((2, 3)),
            pltpu.SemaphoreType.DMA((2, 3)),
            pltpu.SemaphoreType.DMA((2,)),
            pltpu.SemaphoreType.DMA((2,)),
            pltpu.SemaphoreType.DMA((ITERS, count)),
            pltpu.SemaphoreType.DMA((ITERS, count)),
        ],
        compiler_params=pltpu.CompilerParams(collective_id=1, has_side_effects=True, vmem_limit_bytes=32 << 20),
        name="smoothing",
    )(response, weight_field, kappa_field)


def solution(mesh):
    placed = (
        P(("row", "col"), None, None, None),
        P(("row", "col"), None, None, None),
        P(("row", "col"), None, None, None),
        P(("row", "col"), None, None),
        P("row", "col"),
    )
    return jax.shard_map(
        functools.partial(per_device, mesh.shape["row"], mesh.shape["col"]),
        mesh=mesh,
        in_specs=placed,
        out_specs=(P("row", "col"), P("row", "col")),
        check_vma=False,
    )
```

```python
import functools

import jax
import jax.numpy as jnp
from jax import lax
from jax.experimental import pallas as pl
from jax.experimental.pallas import tpu as pltpu
from jax.sharding import PartitionSpec as P

TILE = 128
ITERS = 3
HALO = 8
PAD = 2 * HALO
STRIP = 176
GROUP = 8
LANES = 128
MARGIN = 16
BAND = 16
LIMIT = 2000.0
FOLD = 64
SPAN = TILE * (TILE // FOLD)
ROOM = 59926118

smooth_weight = 0.05

MESH = pl.DeviceIdType.MESH


def greet_all(me, count, cols):
    barrier = pltpu.get_barrier_semaphore()

    def signal(k, carry):
        peer = lax.rem(me + k, count)
        pl.semaphore_signal(
            barrier, inc=1, device_id=(peer // cols, lax.rem(peer, cols)), device_id_type=MESH
        )
        return carry

    lax.fori_loop(1, count, signal, 0)


def await_all(count):
    pl.semaphore_wait(pltpu.get_barrier_semaphore(), count - 1)


def smooth_kernel(
    rows, cols, b_ref, w_ref, k_ref, x_ref, r_ref,
    res, wgt, kap, live, inner, image, along, second, further, course,
    send_low, send_high, recv_low, recv_high, mine, sums,
    row_send, row_recv, col_send, col_recv, sum_send, sum_recv,
):
    count = rows * cols
    my_row, my_col = lax.axis_index("row"), lax.axis_index("col")
    me = my_row * cols + my_col
    height, width = b_ref.shape
    full = width + 128
    own = pl.ds(PAD, height)
    fields = ((b_ref, res), (w_ref, wgt), (k_ref, kap))
    tall = res.shape[0]

    for _, field in fields:
        field[0:PAD, :] = jnp.zeros((PAD, full), jnp.float32)
        field[PAD + height :, :] = jnp.zeros((tall - PAD - height, full), jnp.float32)
    inner[0:HALO, :] = jnp.zeros((HALO, full), jnp.float32)
    inner[PAD + height + HALO : 2 * PAD + height, :] = jnp.zeros((HALO, full), jnp.float32)
    recv_low[...] = jnp.zeros_like(recv_low)
    recv_high[...] = jnp.zeros_like(recv_high)
    greet_all(me, count, cols)

    def fill(i, carry):
        at = pl.multiple_of(i * 32, 32)
        for src, dst in fields:
            dst[pl.ds(PAD + at, 32), 0:width] = src[pl.ds(at, 32), :]
        return carry

    lax.fori_loop(0, height // 32, fill, 0)

    await_all(count)

    up, down = my_row > 0, my_row < rows - 1
    left, right = my_col > 0, my_col < cols - 1

    def row_copies(way):
        made = []
        for at, (src, dst) in enumerate(fields):
            if way == 0:
                source, target = src.at[pl.ds(0, HALO), :], dst.at[pl.ds(PAD + height, HALO), pl.ds(0, width)]
                where = (my_row - 1, my_col)
            else:
                source, target = src.at[pl.ds(height - HALO, HALO), :], dst.at[pl.ds(HALO, HALO), pl.ds(0, width)]
                where = (my_row + 1, my_col)
            made.append(
                pltpu.make_async_remote_copy(
                    src_ref=source, dst_ref=target,
                    send_sem=row_send.at[way, at], recv_sem=row_recv.at[way, at],
                    device_id=where, device_id_type=MESH,
                )
            )
        return made

    def col_copy(way):
        source, target, where = (
            (send_low, recv_high, (my_row, my_col - 1)),
            (send_high, recv_low, (my_row, my_col + 1)),
        )[way]
        return pltpu.make_async_remote_copy(
            src_ref=source, dst_ref=target, send_sem=col_send.at[way], recv_sem=col_recv.at[way],
            device_id=where, device_id_type=MESH,
        )

    for way, there in ((0, up), (1, down)):

        @pl.when(there)
        def _(way=way):
            for copy in row_copies(way):
                copy.start()

    for way, there in ((0, up), (1, down)):

        @pl.when(there)
        def _(way=way):
            for copy in row_copies(way):
                copy.wait_send()

        @pl.when((down, up)[way])
        def _(way=way):
            for copy in row_copies(way):
                copy.wait_recv()

    def pack(i, carry):
        at = pl.multiple_of(i * 128, 128)
        for which, (_, field) in enumerate(fields):
            low = field[pl.ds(at, 128), 0:128].T
            send_low[which * HALO : (which + 1) * HALO, pl.ds(at, 128)] = low[:HALO]
            high = field[pl.ds(at, 128), width - 128 : width].T
            send_high[which * HALO : (which + 1) * HALO, pl.ds(at, 128)] = high[128 - HALO :]
        return carry

    lax.fori_loop(0, tall // 128, pack, 0, unroll=True)
    for way, there in ((0, left), (1, right)):

        @pl.when(there)
        def _(way=way):
            col_copy(way).start()

    for way, there in ((0, left), (1, right)):

        @pl.when(there)
        def _(way=way):
            col_copy(way).wait_send()

        @pl.when((right, left)[way])
        def _(way=way):
            col_copy(way).wait_recv()

    gap = jnp.zeros((128 - 2 * HALO, 128), jnp.float32)

    def unpack(i, carry):
        at = pl.multiple_of(i * 128, 128)
        for which, (_, field) in enumerate(fields):
            part = slice(which * HALO, (which + 1) * HALO)
            both = jnp.concatenate(
                [recv_high[part, pl.ds(at, 128)], gap, recv_low[part, pl.ds(at, 128)]], axis=0
            )
            field[pl.ds(at, 128), width:full] = both.T
        return carry

    lax.fori_loop(0, tall // 128, unpack, 0, unroll=True)

    strips = (height + 2 * HALO) // STRIP
    top = jnp.where(up, HALO, PAD)
    bottom = PAD + height + jnp.where(down, HALO, 0)
    high_end = width + jnp.where(right, HALO, 0)
    low_begin = full - jnp.where(left, HALO, 0)

    def start_of(i):
        return pl.multiple_of(HALO + i * STRIP, 8)

    def prepare(i, carry):
        at = start_of(i)
        row = lax.broadcasted_iota(jnp.int32, (STRIP, full), 0) + at
        col = lax.broadcasted_iota(jnp.int32, (STRIP, full), 1)
        inside = (row >= top) & (row < bottom) & ((col < high_end) | (col >= low_begin))
        mask = jnp.where(inside, 1.0, 0.0).astype(jnp.float32)
        live[pl.ds(at, STRIP), :] = mask
        kap[pl.ds(at, STRIP), :] = jnp.where(inside, 4.0 + kap[pl.ds(at, STRIP), :], 0.0)
        return carry

    lax.fori_loop(0, strips, prepare, 0)

    def stencil(field, at):
        slab = field[pl.ds(pl.multiple_of(at - HALO, 8), STRIP + 2 * HALO), :]
        center = slab[HALO : HALO + STRIP]
        beside = slab[HALO + 1 : HALO + 1 + STRIP] + slab[HALO - 1 : HALO - 1 + STRIP]
        beside = beside + pltpu.roll(center, full - 1, axis=1) + pltpu.roll(center, 1, axis=1)
        here = pl.ds(at, STRIP)
        return kap[here, :] * center - live[here, :] * beside

    def operate(source, target):
        def first(i, carry):
            at = start_of(i)
            inner[pl.ds(at, STRIP), :] = stencil(source, at)
            return carry

        def last(i, carry):
            at = start_of(i)
            here = pl.ds(at, STRIP)
            target[here, :] = wgt[here, :] * source[here, :] + smooth_weight * stencil(inner, at)
            return carry

        lax.fori_loop(0, strips, first, 0)
        lax.fori_loop(0, strips, last, 0)

    lane = lax.broadcasted_iota(jnp.int32, (1, 128), 1)

    def copy_to(step, k, peer, slot):
        return pltpu.make_async_remote_copy(
            src_ref=mine.at[step], dst_ref=sums.at[step, slot],
            send_sem=sum_send.at[step, k], recv_sem=sum_recv.at[step, k],
            device_id=(peer // cols, lax.rem(peer, cols)), device_id_type=MESH,
        )

    def begin_products(step):
        def add(i, carry):
            norm, curve = carry
            here = pl.ds(pl.multiple_of(PAD + i * 32, 8), 32)
            a, c = res[here, 0:width], image[here, 0:width]
            aa, ac = a * a, a * c
            norm = norm + ((aa[:8] + aa[8:16]) + (aa[16:24] + aa[24:]))
            return norm, curve + ((ac[:8] + ac[8:16]) + (ac[16:24] + ac[24:]))

        zero = jnp.zeros((8, width), jnp.float32)
        norm, curve = lax.fori_loop(0, height // 32, add, (zero, zero))
        norm = jnp.sum(jnp.sum(norm, axis=0, keepdims=True), axis=1, keepdims=True)
        curve = jnp.sum(jnp.sum(curve, axis=0, keepdims=True), axis=1, keepdims=True)
        both = jnp.where(lane == 0, norm, jnp.where(lane == 1, curve, 0.0))
        mine[step] = both
        sums[step, me] = both

        def begin(k, carry):
            copy_to(step, k, lax.rem(me + k, count), me).start()
            return carry

        lax.fori_loop(1, count, begin, 0, unroll=True)

    def end_products(step):
        def finish(k, carry):
            source = lax.rem(me + count - k, count)
            copy_to(step, k, source, source).wait()
            return carry

        lax.fori_loop(1, count, finish, 0, unroll=True)
        total = jnp.sum(sums[step], axis=0)
        norm = jnp.sum(jnp.where(lane == 0, total, 0.0), axis=1, keepdims=True)
        curve = jnp.sum(jnp.where(lane == 1, total, 0.0), axis=1, keepdims=True)
        return norm, curve

    operate(res, image)
    begin_products(0)
    norm_now = alpha = None
    for step in range(ITERS):
        if step + 1 < ITERS:
            operate(image, second)
        norm_next, curvature = end_products(step)
        if step == 0:
            ratio = None
            alpha = norm_next / curvature
        else:
            ratio = norm_next / norm_now
            alpha = norm_next / (curvature - ratio * norm_next / alpha)
        norm_now = norm_next

        if step + 1 < ITERS:

            def recede(i, carry, step=step, ratio=ratio, alpha=alpha):
                here = pl.ds(pl.multiple_of(HALO + i * 48, 8), 48)
                way, path, next_path = res[here, :], image[here, :], second[here, :]
                old, old_image = way, path
                if step > 0:
                    way = way + ratio * course[here, :]
                    path = path + ratio * along[here, :]
                    next_path = next_path + ratio * further[here, :]
                course[here, :] = way
                along[here, :] = path
                further[here, :] = next_path
                res[here, :] = old - alpha * path
                image[here, :] = old_image - alpha * next_path
                return carry

            lax.fori_loop(0, (height + 2 * HALO) // 48, recede, 0)
            begin_products(step + 1)

        def advance(i, carry, step=step, ratio=ratio, alpha=alpha):
            at = pl.multiple_of(i * 32, 32)
            here = pl.ds(pl.multiple_of(PAD + at, 8), 32)
            rows_here = pl.ds(at, 32)
            if step + 1 < ITERS:
                moved = alpha * course[here, 0:width]
            else:
                moved = alpha * (res[here, 0:width] + ratio * course[here, 0:width])
                r_ref[rows_here, :] = res[here, 0:width] - alpha * (
                    image[here, 0:width] + ratio * along[here, 0:width]
                )
            x_ref[rows_here, :] = moved if step == 0 else x_ref[rows_here, :] + moved
            return carry

        lax.fori_loop(0, height // 32, advance, 0)


def edge_and_inner(down, across):
    edge = 2 * across + 2 * (down - 2)
    return edge, (down - 2) * (across - 2)


def edge_tile(e, down, across):
    side = e - across
    last = across + 2 * (down - 2)
    row = jnp.where(e < across, 0, jnp.where(e < last, 1 + side // 2, down - 1))
    col = jnp.where(e < across, e, jnp.where(e < last, lax.rem(side, 2) * (across - 1), e - last))
    return row, col


def inner_tile(e, down, across):
    return 1 + e // (across - 2), 1 + lax.rem(e, across - 2)


def split(value, size):
    if size & (size - 1) == 0:
        return lax.shift_right_logical(value, size.bit_length() - 1), value & (size - 1)
    return lax.div(value, size), lax.rem(value, size)


def digit_steps(place, size):
    return [(1 << n) * (1 - 2 * lax.rem(place // (1 << n), 2)) for n in range(size.bit_length() - 1)]


def flip(place, steps, code):
    for n, step in enumerate(steps):
        if code >> n & 1:
            place = place + step
    return place


def field_kernel(
    rows, cols, cell_hbm, value_hbm, weight_hbm, count_hbm, kappa_hbm,
    fields, coef, good,
    cell_in, value_in, weight_in, count_in, cell_wide, value_wide, weight_wide,
    code_out, pair_out, code_out_inner, pair_out_inner,
    code_in, pair_in, code_in_inner, pair_in_inner,
    place_row, place_col, amounts, kap, mid,
    low_out, high_out, low_in, high_in, kap_low_out, kap_high_out, kap_low_in, kap_high_in,
    mine, sums,
    load_sems, send_sem, recv_sems, halo_send, halo_recv, sum_sems,
):
    bw, first, second, third = fields.at[0:2], fields.at[2], fields.at[3], fields.at[4]
    count = rows * cols
    my_row, my_col = lax.axis_index("row"), lax.axis_index("col")
    me = my_row * cols + my_col
    height, width = kappa_hbm.shape
    down, across = height // TILE, width // TILE
    tiles = down * across
    slots = code_in.shape[2]
    edges, inners = edge_and_inner(down, across)
    pitch = cell_wide.shape[0] // tiles
    bottom = MARGIN + height
    lane = lax.broadcasted_iota(jnp.int32, (1, LANES), 1)

    loads = [
        pltpu.make_async_copy(cell_hbm, cell_in, load_sems.at[0]),
        pltpu.make_async_copy(value_hbm, value_in, load_sems.at[1]),
        pltpu.make_async_copy(weight_hbm, weight_in, load_sems.at[2]),
        pltpu.make_async_copy(count_hbm, count_in, load_sems.at[3]),
    ]
    kappa_loads = [
        pltpu.make_async_copy(
            kappa_hbm.at[:, pl.ds(c * LANES, LANES)], kap.at[c, pl.ds(MARGIN, height), :], load_sems.at[4 + c]
        )
        for c in range(across)
    ]
    for load in loads + kappa_loads:
        load.start()

    for ref in (low_in, high_in, kap_low_in, kap_high_in):
        ref[...] = jnp.zeros_like(ref)
    strip = jnp.zeros((MARGIN, LANES), jnp.float32)
    for c in range(across):
        for field in (bw.at[0], bw.at[1], kap):
            field[c, 0:MARGIN, :] = strip
            field[c, bottom : bottom + MARGIN, :] = strip

    row_steps, col_steps = digit_steps(my_row, rows), digit_steps(my_col, cols)

    def person(k):
        return flip(my_row, row_steps, k % rows), flip(my_col, col_steps, k // rows)

    barrier = pltpu.get_barrier_semaphore()
    with jax.named_scope("greet"):
        for k in reversed(range(1, count)):
            pl.semaphore_signal(barrier, inc=1, device_id=person(k), device_id_type=MESH)

    for field in (bw.at[0], bw.at[1], kap):
        field[across, 0:MARGIN, :] = strip
        field[across, bottom : bottom + MARGIN, :] = strip
    for c in range(across + 1):
        for field in (mid, first, second):
            field[c, 0:8, :] = strip[:8]
            field[c, bottom + 8 : bottom + 16, :] = strip[:8]


    with jax.named_scope("loads"):
        for load in loads:
            load.wait()

    def widen(t, carry):
        here = pl.ds(pl.multiple_of(t * count, 8), count)
        there = pl.ds(pl.multiple_of(t * pitch, 8), count)
        cell_wide[there, :] = cell_in[here, :]
        weight = weight_in[here, :].astype(jnp.float32)
        weight_wide[there, :] = weight
        value_wide[there, :] = weight * value_in[here, :].astype(jnp.float32)
        return carry

    with jax.named_scope("widen"):
        lax.fori_loop(0, tiles, widen, 0)
    dest_lane = lax.broadcasted_iota(jnp.int32, count_in.shape, 1)
    counts = count_in[...].astype(jnp.float32)
    slot_lane = lax.broadcasted_iota(jnp.int32, (tiles, slots), 1).astype(jnp.float32)
    edge_ids = [t for t in range(tiles) if t // across in (0, down - 1) or t % across in (0, across - 1)]
    inner_ids = [t for t in range(tiles) if t not in edge_ids]

    def pick(value, ids):
        parts, begin = [], 0
        while begin < len(ids):
            end = begin
            while end + 1 < len(ids) and ids[end + 1] == ids[end] + 1:
                end += 1
            parts.append(value[ids[begin] : ids[end] + 1])
            begin = end + 1
        return jnp.concatenate(parts, axis=0) if len(parts) > 1 else parts[0]

    def encode(k):
        row, col = person(k)
        dest = row * cols + col
        every = pl.ds(dest, tiles, stride=pitch)
        cell = cell_wide[every, :]
        upper, _ = split(cell, width * cols)
        line = split(upper, TILE)[1]
        side, place = split(line, FOLD)
        local = place * SPAN + side * TILE + split(cell, TILE)[1]
        alive = jnp.sum(jnp.where(dest_lane == dest, counts, 0.0), axis=1, keepdims=True)
        local = jnp.where(slot_lane < alive, local, -1)
        weight, product = weight_wide[every, :], value_wide[every, :]
        code_out[k] = pick(local, edge_ids).astype(jnp.int16)
        pair_out[k] = jnp.concatenate([pick(weight, edge_ids), pick(product, edge_ids)], axis=0).astype(jnp.bfloat16)
        code_out_inner[k] = pick(local, inner_ids).astype(jnp.int16)
        pair_out_inner[k] = jnp.concatenate(
            [pick(weight, inner_ids), pick(product, inner_ids)], axis=0
        ).astype(jnp.bfloat16)

    with jax.named_scope("encode"):
        for k in reversed(range(count)):
            encode(k)
    pieces = (
        ((code_out, code_in), (pair_out, pair_in), edges, edge_tile),
        ((code_out_inner, code_in_inner), (pair_out_inner, pair_in_inner), inners, inner_tile),
    )
    for piece in pieces:
        for source, target in piece[:2]:
            target[0] = source[0]
    with jax.named_scope("arrive"):
        await_all(count)

    bunch = GROUP
    chunks = count // bunch

    def send(piece, begin, end):
        for k in range(begin, end):
            place = person(k)
            for which, (source, target) in enumerate(pieces[piece][:2]):
                pltpu.make_async_remote_copy(
                    src_ref=source.at[k], dst_ref=target.at[k],
                    send_sem=send_sem.at[piece, which], recv_sem=recv_sems.at[k // bunch, piece, which],
                    device_id=place, device_id_type=MESH,
                ).start()

    half = count // 2
    with jax.named_scope("send"):
        send(0, half, count)
        send(0, 1, half)
        send(1, 1, half)
        send(1, half, count)

    def halo_copies(group, body, parts):
        low_from, high_from, low_to, high_to = parts
        up_rows, down_rows = pl.ds(MARGIN, 8), pl.ds(bottom - 8, 8)
        above, below = pl.ds(MARGIN - 8, 8), pl.ds(bottom, 8)
        main = pl.ds(LANES, height)
        head, tail = pl.ds(0, LANES), pl.ds(LANES + height, LANES)
        begin, end = pl.ds(0, LANES), pl.ds(height - LANES, LANES)
        whole = pl.ds(0, height)
        plan = [
            (-1, 0, body(up_rows), body(below)),
            (1, 0, body(down_rows), body(above)),
            (0, -1, low_from.at[:, whole], high_to.at[:, main]),
            (0, 1, high_from.at[:, whole], low_to.at[:, main]),
            (-1, -1, low_from.at[:, begin], high_to.at[:, tail]),
            (1, -1, low_from.at[:, end], high_to.at[:, head]),
            (-1, 1, high_from.at[:, begin], low_to.at[:, tail]),
            (1, 1, high_from.at[:, end], low_to.at[:, head]),
        ]
        made = []
        for at, (dr, dc, source, target) in enumerate(plan):

            def there(dr=dr, dc=dc):
                ok = True
                for step, place, size in ((dr, my_row, rows), (dc, my_col, cols)):
                    if step < 0:
                        ok = (place > 0) & ok
                    if step > 0:
                        ok = (place < size - 1) & ok
                return ok

            copy = pltpu.make_async_remote_copy(
                src_ref=source, dst_ref=target,
                send_sem=halo_send.at[group, at], recv_sem=halo_recv.at[group, at],
                device_id=(my_row + dr, my_col + dc), device_id_type=MESH,
            )
            made.append((there(), there(-dr, -dc), copy))
        return made

    def start_halo(copies):
        for goes, _, copy in copies:

            @pl.when(goes)
            def _(copy=copy):
                copy.start()

    def end_halo(copies):
        for goes, comes, copy in copies:

            @pl.when(goes)
            def _(copy=copy):
                copy.wait_send()

            @pl.when(comes)
            def _(copy=copy):
                copy.wait_recv()

    def pack(field, at, low, high):
        for j in range(down):
            here = pl.ds(MARGIN + j * TILE, TILE)
            there = slice(j * TILE, (j + 1) * TILE)
            low[at : at + 8, there] = field[0, here, :].T[:8]
            high[at : at + 8, there] = field[across - 1, here, :].T[TILE - 8 :]

    gap = jnp.zeros((LANES - 16, LANES), jnp.float32)

    def unpack(field, at, low, high):
        for j in range(-1, down + 1):
            lanes = slice(LANES + j * TILE, LANES + (j + 1) * TILE)
            both = jnp.concatenate([high[at : at + 8, lanes], gap, low[at : at + 8, lanes]], axis=0).T
            if j < 0:
                field[across, MARGIN - 8 : MARGIN, :] = both[TILE - 8 :]
            elif j == down:
                field[across, bottom : bottom + 8, :] = both[:8]
            else:
                field[across, MARGIN + j * TILE : MARGIN + (j + 1) * TILE, :] = both

    kap_halo = halo_copies(
        0, lambda part: kap.at[pl.ds(0, across), part, :], (kap_low_out, kap_high_out, kap_low_in, kap_high_in)
    )
    bw_halo = halo_copies(
        1, lambda part: bw.at[:, pl.ds(0, across), part, :], (low_out, high_out, low_in, high_in)
    )
    with jax.named_scope("kappa"):
        for load in kappa_loads:
            load.wait()
        pack(kap, 0, kap_low_out, kap_high_out)
        start_halo(kap_halo)

    offsets = lax.broadcasted_iota(jnp.int32, (SPAN, slots), 0).astype(jnp.float32).astype(jnp.bfloat16)
    one = jnp.ones((SPAN, slots), jnp.bfloat16)
    zero = jnp.zeros((SPAN, slots), jnp.bfloat16)

    def bin_chunk(chunk, piece):
        codes, pairs, some, locate = pieces[piece]
        for which, (_, target) in enumerate((codes, pairs)):
            begin = chunk * bunch + (1 if chunk == 0 else 0)
            part = target.at[pl.ds(begin, (chunk + 1) * bunch - begin)]
            with jax.named_scope(f"wait{piece}"):
                pltpu.make_async_copy(part, part, recv_sems.at[chunk, piece, which]).wait()
        with jax.named_scope("spread"):
            for n in range(bunch):
                code = codes[1][chunk * bunch + n].astype(jnp.int32)
                place_row[n * some : (n + 1) * some, :] = (code >> (SPAN.bit_length() - 1)).astype(jnp.float32)
                place_col[n * some : (n + 1) * some, :] = (code & (SPAN - 1)).astype(jnp.float32)
                amounts[n * 2 * some : (n + 1) * 2 * some, :] = pairs[1][chunk * bunch + n].astype(jnp.float32)

        def spread(ref, at, size):
            return jnp.broadcast_to(ref[pl.ds(at, 1), :].astype(jnp.bfloat16), (size, slots))

        def bin_tile(e, carry):
            hot, weights, products = [], [], []
            for n in range(bunch):
                hit = spread(place_col, n * some + e, SPAN) == offsets
                hot.append(jnp.where(hit, one, zero).astype(jnp.float8_e4m3fn))
                hit = spread(place_row, n * some + e, FOLD) == offsets[:FOLD]
                weights.append(jnp.where(hit, spread(amounts, n * 2 * some + e, FOLD), zero[:FOLD]))
                products.append(jnp.where(hit, spread(amounts, n * 2 * some + some + e, FOLD), zero[:FOLD]))
            stacked = jnp.concatenate(
                [jnp.concatenate(products, axis=1), jnp.concatenate(weights, axis=1)], axis=0
            )
            total = lax.dot_general(
                stacked, jnp.concatenate(hot, axis=1), (((1,), (1,)), ((), ())),
                preferred_element_type=jnp.float32,
            )
            row, col = locate(e, down, across)
            for n in range(TILE // FOLD):
                here = pl.ds(pl.multiple_of(MARGIN + row * TILE + n * FOLD, 8), FOLD)
                lanes = slice(n * TILE, (n + 1) * TILE)
                for which in range(2):
                    part = total[which * FOLD : (which + 1) * FOLD, lanes]
                    if chunk == 0:
                        bw[which, col, here, :] = part
                    else:
                        bw[which, col, here, :] += part
            return carry

        with jax.named_scope("bin"):
            lax.fori_loop(0, some, bin_tile, 0, unroll=4)

    for chunk in range(chunks // 2):
        bin_chunk(chunk, 0)
        bin_chunk(chunk, 1)
    for chunk in range(chunks // 2, chunks):
        bin_chunk(chunk, 0)
    with jax.named_scope("pack"):
        for which in range(2):
            pack(bw.at[which], 8 * which, low_out, high_out)
        start_halo(bw_halo)
    for chunk in range(chunks // 2, chunks):
        bin_chunk(chunk, 1)
    with jax.named_scope("kap_halo"):
        end_halo(kap_halo)
        unpack(kap, 0, kap_low_in, kap_high_in)

        def lift(i, carry):
            here = pl.ds(pl.multiple_of(i * 16, 8), 16)
            for c in range(across + 1):
                kap[c, here, :] = 4.0 + kap[c, here, :]
            return carry

        lax.fori_loop(0, kap.shape[1] // 16, lift, 0, unroll=2)
    with jax.named_scope("sent"):
        for piece in range(2):
            for which, (source, _) in enumerate(pieces[piece][:2]):
                part = source.at[pl.ds(1, count - 1)]
                pltpu.make_async_copy(part, part, send_sem.at[piece, which]).wait()
    with jax.named_scope("halo"):
        end_halo(bw_halo)
    with jax.named_scope("unpack"):
        for which in range(2):
            unpack(bw.at[which], 8 * which, low_in, high_in)

    up, under = my_row > 0, my_row < rows - 1
    live = ((lane < 8) & (my_col < cols - 1)) | ((lane >= LANES - 8) & (my_col > 0))

    def inner(field, at, size, columns):
        every = range(across + 1)
        here = pl.ds(at, size)
        center = [field[c, here, :] for c in every]
        ahead = [pltpu.roll(x, 1, axis=1) for x in center]
        behind = [pltpu.roll(x, LANES - 1, axis=1) for x in center]
        result = []
        for c in range(columns):
            beside = field[c, pl.ds(at - 1, size), :] + field[c, pl.ds(at + 1, size), :]
            beside = beside + jnp.where(lane == 0, ahead[c - 1], ahead[c])
            beside = beside + jnp.where(lane == LANES - 1, behind[(c + 1) % (across + 1)], behind[c])
            value = kap[c, here, :] * center[c] - beside
            result.append(jnp.where(live, value, 0.0) if c == across else value)
        return result

    response, weight = bw.at[0], bw.at[1]
    outer = ((MARGIN - 8, up), (bottom, under))

    def bands(body, carry):
        def step(i, carry):
            return body(pl.multiple_of(MARGIN + i * BAND, 8), carry)

        return lax.fori_loop(0, height // BAND, step, carry, unroll=8)

    def fold(value):
        total = value[0:8]
        for n in range(8, value.shape[0], 8):
            total = total + value[n : n + 8]
        return total

    def apply_inner(source):
        def body(at, carry):
            square, energy = carry
            for c, value in enumerate(inner(source, at, BAND, across + 1)):
                here = pl.ds(at, BAND)
                mid[c, here, :] = value
                if c < across:
                    x = source[c, here, :]
                    xx = x * x
                    square = square + fold(xx)
                    energy = energy + fold(weight[c, here, :] * xx + smooth_weight * (value * value))
            return square, energy

        blank = jnp.zeros((8, LANES), jnp.float32)
        result = bands(body, (blank, blank))
        for at, there in outer:
            for c, value in enumerate(inner(source, at, 8, across + 1)):
                mid[c, pl.ds(at, 8), :] = jnp.where(there, value, 0.0)
        return result

    def apply_outer(source, target):
        def store(at, size, there=None):
            for c, value in enumerate(inner(mid, at, size, across + 1)):
                here = pl.ds(at, size)
                value = weight[c, here, :] * source[c, here, :] + smooth_weight * value
                target[c, here, :] = value if there is None else jnp.where(there, value, 0.0)

        def body(at, carry):
            store(at, BAND)
            return carry

        bands(body, 0)
        for at, there in outer:
            store(at, 8, there)

    moments = []
    with jax.named_scope("op1"):
        moments += apply_inner(response)
    with jax.named_scope("op2"):
        apply_outer(response, first)
    with jax.named_scope("op3"):
        moments += apply_inner(first)
    with jax.named_scope("op4"):
        apply_outer(first, second)
    with jax.named_scope("op5"):
        moments += apply_inner(second)

    with jax.named_scope("fold"):
        both = jnp.zeros((1, LANES), jnp.float32)
        for at, value in enumerate(moments):
            total = jnp.sum(jnp.sum(value, axis=0, keepdims=True), axis=1, keepdims=True)
            both = jnp.where(lane == at, total, both)
        mine[...] = both
        sums[me] = both

    with jax.named_scope("sum_send"):
        for k in reversed(range(1, count)):
            pltpu.make_async_remote_copy(
                src_ref=mine, dst_ref=sums.at[me],
                send_sem=sum_sems.at[0], recv_sem=sum_sems.at[1],
                device_id=person(k), device_id_type=MESH,
            ).start()

    def last(at, carry):
        for c, value in enumerate(inner(mid, at, BAND, across)):
            here = pl.ds(at, BAND)
            third[c, here, :] = weight[c, here, :] * second[c, here, :] + smooth_weight * value
        return carry

    with jax.named_scope("op6"):
        bands(last, 0)

    with jax.named_scope("sum_wait"):
        part = sums.at[pl.ds(1, count - 1)]
        for n in range(2):
            pltpu.make_async_copy(part, part, sum_sems.at[n]).wait()
    coef_scope = jax.named_scope("coef")
    coef_scope.__enter__()
    total = jnp.sum(sums[...], axis=0)
    m = [jnp.sum(jnp.where(lane == at, total, 0.0), axis=1, keepdims=True) for at in range(6)]
    scale = m[1] / m[0]
    power, n = scale, [None, None]
    for at in range(2, 6):
        power = power * scale
        n.append(m[at] / m[0] / power)
    fall = n[2] - 1.0
    bend = n[3] - n[2] * n[2]
    alpha = fall / bend
    a = 1.0 + alpha * n[2]
    lead = n[2] - a * n[3] + alpha * n[4]
    lead_size = n[2] + a * n[3] + alpha * n[4]
    beta = alpha * lead / fall
    d0, d1 = 1.0 + beta * n[2], a + beta
    turn = d0 * n[3] - d1 * n[4] + alpha * n[5]
    turn_size = d0 * n[3] + d1 * n[4] + alpha * n[5]
    step = lead / turn
    inverse = 1.0 / scale
    powers = [inverse, inverse * inverse, inverse * inverse * inverse]
    parts = [
        (1.0 + alpha * n[2] + step * d0) * powers[0],
        -(alpha + step * d1) * powers[1],
        step * alpha * powers[2],
        -(a + step * d0) * powers[0],
        (alpha + step * d1) * powers[1],
        -(step * alpha) * powers[2],
    ]
    for at, value in enumerate(parts):
        coef[at : at + 1, :] = jnp.broadcast_to(value, (1, LANES))
    coef[6:8, :] = jnp.zeros((2, LANES), jnp.float32)
    sound = (fall * LIMIT >= n[2]) & (bend * LIMIT >= n[3])
    sound = sound & (lead * LIMIT >= lead_size) & (turn * LIMIT >= turn_size)
    sound = sound & (alpha * lead * (2.0 * LIMIT) >= 1.0 + a * a * n[2] + alpha * alpha * n[4])
    good[...] = jnp.where(sound, 1, 0)
    coef_scope.__exit__(None, None, None)


def combine_kernel(fields, coef, x_hbm, r_hbm, x_out, r_out, sems):
    height, width = x_hbm.shape
    across = width // LANES
    band = height // 8
    weights = [coef[at : at + 1, :] for at in range(6)]
    copies = []
    for i in range(8):
        rows_here = pl.ds(i * band, band)

        def body(j, carry, i=i):
            at = pl.multiple_of(i * band + j * 32, 8)
            for c in range(across):
                here = pl.ds(MARGIN + at, 32)
                values = [fields[n, c, here, :] for n in (0, 2, 3, 4)]
                lanes = slice(c * LANES, (c + 1) * LANES)
                x_out[pl.ds(at, 32), lanes] = (
                    weights[0] * values[0] + weights[1] * values[1] + weights[2] * values[2]
                )
                r_out[pl.ds(at, 32), lanes] = (
                    values[0] + weights[3] * values[1] + weights[4] * values[2] + weights[5] * values[3]
                )
            return carry

        lax.fori_loop(0, band // 32, body, 0)
        for at, (source, target) in enumerate(((x_out, x_hbm), (r_out, r_hbm))):
            copy = pltpu.make_async_copy(source.at[rows_here], target.at[rows_here], sems.at[i, at])
            copy.start()
            copies.append(copy)
    for copy in copies:
        copy.wait()


def copy_kernel(x_in, r_in, x_out, r_out):
    x_out[...] = x_in[...]
    r_out[...] = r_in[...]


def per_device(rows, cols, obs_cell, obs_value, obs_weight, obs_count, kappa_field):
    count = rows * cols
    height, width = kappa_field.shape
    tiles, _, slots = obs_cell.shape[1:]
    down, across = height // TILE, width // TILE
    edges, inners = edge_and_inner(down, across)
    in_vmem = pl.BlockSpec(memory_space=pltpu.VMEM)
    in_hbm = pl.BlockSpec(memory_space=pltpu.HBM)
    tall = height + 2 * MARGIN
    field = jax.ShapeDtypeStruct((height, width), jnp.float32)
    wide = jax.ShapeDtypeStruct((across + 1, tall, LANES), jnp.float32)
    pitch = count + 8
    flat = (tiles * count, slots)
    pitched = (tiles * pitch, slots)
    edge = [
        pltpu.VMEM((count, edges, slots), jnp.int16),
        pltpu.VMEM((count, 2 * edges, slots), jnp.bfloat16),
        pltpu.VMEM((count, inners, slots), jnp.int16),
        pltpu.VMEM((count, 2 * inners, slots), jnp.bfloat16),
    ]
    fields, coef, good = pl.pallas_call(
        functools.partial(field_kernel, rows, cols),
        out_shape=(
            jax.ShapeDtypeStruct((5, across + 1, tall, LANES), jnp.float32),
            jax.ShapeDtypeStruct((8, LANES), jnp.float32),
            jax.ShapeDtypeStruct((1, 1), jnp.int32),
        ),
        in_specs=[in_hbm] * 5,
        out_specs=(in_vmem,) * 3,
        scratch_shapes=[
            pltpu.VMEM(flat, jnp.int32),
            pltpu.VMEM(flat, jnp.bfloat16),
            pltpu.VMEM(flat, jnp.bfloat16),
            pltpu.VMEM((tiles, count), jnp.int32),
            pltpu.VMEM(pitched, jnp.int32),
            pltpu.VMEM(pitched, jnp.float32),
            pltpu.VMEM(pitched, jnp.float32),
            *edge,
            *edge,
            pltpu.VMEM((GROUP * edges, slots), jnp.float32),
            pltpu.VMEM((GROUP * edges, slots), jnp.float32),
            pltpu.VMEM((GROUP * edges * 2, slots), jnp.float32),
            pltpu.VMEM(wide.shape, jnp.float32),
            pltpu.VMEM(wide.shape, jnp.float32),
            pltpu.VMEM((16, height), jnp.float32),
            pltpu.VMEM((16, height), jnp.float32),
            pltpu.VMEM((16, height + 2 * LANES), jnp.float32),
            pltpu.VMEM((16, height + 2 * LANES), jnp.float32),
            pltpu.VMEM((8, height), jnp.float32),
            pltpu.VMEM((8, height), jnp.float32),
            pltpu.VMEM((8, height + 2 * LANES), jnp.float32),
            pltpu.VMEM((8, height + 2 * LANES), jnp.float32),
            pltpu.VMEM((1, LANES), jnp.float32),
            pltpu.VMEM((count, 1, LANES), jnp.float32),
            pltpu.SemaphoreType.DMA((4 + across,)),
            pltpu.SemaphoreType.DMA((2, 2)),
            pltpu.SemaphoreType.DMA((count // GROUP, 2, 2)),
            pltpu.SemaphoreType.DMA((2, 8)),
            pltpu.SemaphoreType.DMA((2, 8)),
            pltpu.SemaphoreType.DMA((2,)),
        ],
        compiler_params=pltpu.CompilerParams(
            collective_id=0, has_side_effects=True, vmem_limit_bytes=ROOM
        ),
        name="fields",
    )(
        obs_cell.reshape(flat), obs_value.reshape(flat), obs_weight.reshape(flat),
        obs_count[0], kappa_field,
    )

    def combine(fields, coef, *unused):
        return pl.pallas_call(
            combine_kernel,
            out_shape=(field, field),
            in_specs=[in_vmem] * 2,
            out_specs=(in_hbm,) * 2,
            scratch_shapes=[
                pltpu.VMEM(field.shape, jnp.float32),
                pltpu.VMEM(field.shape, jnp.float32),
                pltpu.SemaphoreType.DMA((8, 2)),
            ],
            compiler_params=pltpu.CompilerParams(vmem_limit_bytes=16 << 20),
            name="combine",
        )(fields, coef)

    def iterate(fields, coef, kappa):
        own = fields[:2, :across, MARGIN : MARGIN + height, :].transpose(0, 2, 1, 3).reshape(2, height, width)
        return pl.pallas_call(
            copy_kernel,
            out_shape=(field, field),
            in_specs=[in_vmem] * 2,
            out_specs=(in_vmem,) * 2,
            name="hand_on",
        )(*smooth(rows, cols, own[0], own[1], kappa))

    return lax.cond(good[0, 0] > 0, combine, iterate, fields, coef, kappa_field)


def smooth(rows, cols, response, weight_field, kappa_field):
    count = rows * cols
    height, width = kappa_field.shape
    in_vmem = pl.BlockSpec(memory_space=pltpu.VMEM)
    field = jax.ShapeDtypeStruct((height, width), jnp.float32)
    full = width + 128
    tall = -(-(height + 2 * PAD) // 128) * 128
    extended = pltpu.VMEM((tall, full), jnp.float32)
    edge = pltpu.VMEM((3 * HALO, tall), jnp.float32)
    return pl.pallas_call(
        functools.partial(smooth_kernel, rows, cols),
        out_shape=(field, field),
        in_specs=[in_vmem] * 3,
        out_specs=(in_vmem,) * 2,
        scratch_shapes=[extended] * 10
        + [edge] * 4
        + [
            pltpu.VMEM((ITERS, 1, 128), jnp.float32),
            pltpu.VMEM((ITERS, count, 1, 128), jnp.float32),
            pltpu.SemaphoreType.DMA((2, 3)),
            pltpu.SemaphoreType.DMA((2, 3)),
            pltpu.SemaphoreType.DMA((2,)),
            pltpu.SemaphoreType.DMA((2,)),
            pltpu.SemaphoreType.DMA((ITERS, count)),
            pltpu.SemaphoreType.DMA((ITERS, count)),
        ],
        compiler_params=pltpu.CompilerParams(collective_id=1, has_side_effects=True, vmem_limit_bytes=32 << 20),
        name="smoothing",
    )(response, weight_field, kappa_field)


def solution(mesh):
    placed = (
        P(("row", "col"), None, None, None),
        P(("row", "col"), None, None, None),
        P(("row", "col"), None, None, None),
        P(("row", "col"), None, None),
        P("row", "col"),
    )
    return jax.shard_map(
        functools.partial(per_device, mesh.shape["row"], mesh.shape["col"]),
        mesh=mesh,
        in_specs=placed,
        out_specs=(P("row", "col"), P("row", "col")),
        check_vma=False,
    )
```

```python
import functools

import jax
import jax.numpy as jnp
from jax import lax
from jax.experimental import pallas as pl
from jax.experimental.pallas import tpu as pltpu
from jax.sharding import PartitionSpec as P

TILE = 128
ITERS = 3
HALO = 8
PAD = 2 * HALO
STRIP = 176
GROUP = 8
LANES = 128
MARGIN = 16
BAND = 16
LIMIT = 1000.0
UNROLL = 32
TILES_AT_ONCE = 4
FOLD = 64
SPAN = TILE * (TILE // FOLD)
ROOM = 59926118

smooth_weight = 0.05

MESH = pl.DeviceIdType.MESH


def greet_all(me, count, cols):
    barrier = pltpu.get_barrier_semaphore()

    def signal(k, carry):
        peer = lax.rem(me + k, count)
        pl.semaphore_signal(
            barrier, inc=1, device_id=(peer // cols, lax.rem(peer, cols)), device_id_type=MESH
        )
        return carry

    lax.fori_loop(1, count, signal, 0)


def await_all(count):
    pl.semaphore_wait(pltpu.get_barrier_semaphore(), count - 1)


def smooth_kernel(
    rows, cols, b_ref, w_ref, k_ref, x_ref, r_ref,
    res, wgt, kap, live, inner, image, along, second, further, course,
    send_low, send_high, recv_low, recv_high, mine, sums,
    row_send, row_recv, col_send, col_recv, sum_send, sum_recv,
):
    count = rows * cols
    my_row, my_col = lax.axis_index("row"), lax.axis_index("col")
    me = my_row * cols + my_col
    height, width = b_ref.shape
    full = width + 128
    own = pl.ds(PAD, height)
    fields = ((b_ref, res), (w_ref, wgt), (k_ref, kap))
    tall = res.shape[0]

    for _, field in fields:
        field[0:PAD, :] = jnp.zeros((PAD, full), jnp.float32)
        field[PAD + height :, :] = jnp.zeros((tall - PAD - height, full), jnp.float32)
    inner[0:HALO, :] = jnp.zeros((HALO, full), jnp.float32)
    inner[PAD + height + HALO : 2 * PAD + height, :] = jnp.zeros((HALO, full), jnp.float32)
    recv_low[...] = jnp.zeros_like(recv_low)
    recv_high[...] = jnp.zeros_like(recv_high)
    greet_all(me, count, cols)

    def fill(i, carry):
        at = pl.multiple_of(i * 32, 32)
        for src, dst in fields:
            dst[pl.ds(PAD + at, 32), 0:width] = src[pl.ds(at, 32), :]
        return carry

    lax.fori_loop(0, height // 32, fill, 0)

    await_all(count)

    up, down = my_row > 0, my_row < rows - 1
    left, right = my_col > 0, my_col < cols - 1

    def row_copies(way):
        made = []
        for at, (src, dst) in enumerate(fields):
            if way == 0:
                source, target = src.at[pl.ds(0, HALO), :], dst.at[pl.ds(PAD + height, HALO), pl.ds(0, width)]
                where = (my_row - 1, my_col)
            else:
                source, target = src.at[pl.ds(height - HALO, HALO), :], dst.at[pl.ds(HALO, HALO), pl.ds(0, width)]
                where = (my_row + 1, my_col)
            made.append(
                pltpu.make_async_remote_copy(
                    src_ref=source, dst_ref=target,
                    send_sem=row_send.at[way, at], recv_sem=row_recv.at[way, at],
                    device_id=where, device_id_type=MESH,
                )
            )
        return made

    def col_copy(way):
        source, target, where = (
            (send_low, recv_high, (my_row, my_col - 1)),
            (send_high, recv_low, (my_row, my_col + 1)),
        )[way]
        return pltpu.make_async_remote_copy(
            src_ref=source, dst_ref=target, send_sem=col_send.at[way], recv_sem=col_recv.at[way],
            device_id=where, device_id_type=MESH,
        )

    for way, there in ((0, up), (1, down)):

        @pl.when(there)
        def _(way=way):
            for copy in row_copies(way):
                copy.start()

    for way, there in ((0, up), (1, down)):

        @pl.when(there)
        def _(way=way):
            for copy in row_copies(way):
                copy.wait_send()

        @pl.when((down, up)[way])
        def _(way=way):
            for copy in row_copies(way):
                copy.wait_recv()

    def pack(i, carry):
        at = pl.multiple_of(i * 128, 128)
        for which, (_, field) in enumerate(fields):
            low = field[pl.ds(at, 128), 0:128].T
            send_low[which * HALO : (which + 1) * HALO, pl.ds(at, 128)] = low[:HALO]
            high = field[pl.ds(at, 128), width - 128 : width].T
            send_high[which * HALO : (which + 1) * HALO, pl.ds(at, 128)] = high[128 - HALO :]
        return carry

    lax.fori_loop(0, tall // 128, pack, 0, unroll=True)
    for way, there in ((0, left), (1, right)):

        @pl.when(there)
        def _(way=way):
            col_copy(way).start()

    for way, there in ((0, left), (1, right)):

        @pl.when(there)
        def _(way=way):
            col_copy(way).wait_send()

        @pl.when((right, left)[way])
        def _(way=way):
            col_copy(way).wait_recv()

    gap = jnp.zeros((128 - 2 * HALO, 128), jnp.float32)

    def unpack(i, carry):
        at = pl.multiple_of(i * 128, 128)
        for which, (_, field) in enumerate(fields):
            part = slice(which * HALO, (which + 1) * HALO)
            both = jnp.concatenate(
                [recv_high[part, pl.ds(at, 128)], gap, recv_low[part, pl.ds(at, 128)]], axis=0
            )
            field[pl.ds(at, 128), width:full] = both.T
        return carry

    lax.fori_loop(0, tall // 128, unpack, 0, unroll=True)

    strips = (height + 2 * HALO) // STRIP
    top = jnp.where(up, HALO, PAD)
    bottom = PAD + height + jnp.where(down, HALO, 0)
    high_end = width + jnp.where(right, HALO, 0)
    low_begin = full - jnp.where(left, HALO, 0)

    def start_of(i):
        return pl.multiple_of(HALO + i * STRIP, 8)

    def prepare(i, carry):
        at = start_of(i)
        row = lax.broadcasted_iota(jnp.int32, (STRIP, full), 0) + at
        col = lax.broadcasted_iota(jnp.int32, (STRIP, full), 1)
        inside = (row >= top) & (row < bottom) & ((col < high_end) | (col >= low_begin))
        mask = jnp.where(inside, 1.0, 0.0).astype(jnp.float32)
        live[pl.ds(at, STRIP), :] = mask
        kap[pl.ds(at, STRIP), :] = jnp.where(inside, 4.0 + kap[pl.ds(at, STRIP), :], 0.0)
        return carry

    lax.fori_loop(0, strips, prepare, 0)

    def stencil(field, at):
        slab = field[pl.ds(pl.multiple_of(at - HALO, 8), STRIP + 2 * HALO), :]
        center = slab[HALO : HALO + STRIP]
        beside = slab[HALO + 1 : HALO + 1 + STRIP] + slab[HALO - 1 : HALO - 1 + STRIP]
        beside = beside + pltpu.roll(center, full - 1, axis=1) + pltpu.roll(center, 1, axis=1)
        here = pl.ds(at, STRIP)
        return kap[here, :] * center - live[here, :] * beside

    def operate(source, target):
        def first(i, carry):
            at = start_of(i)
            inner[pl.ds(at, STRIP), :] = stencil(source, at)
            return carry

        def last(i, carry):
            at = start_of(i)
            here = pl.ds(at, STRIP)
            target[here, :] = wgt[here, :] * source[here, :] + smooth_weight * stencil(inner, at)
            return carry

        lax.fori_loop(0, strips, first, 0)
        lax.fori_loop(0, strips, last, 0)

    lane = lax.broadcasted_iota(jnp.int32, (1, 128), 1)

    def copy_to(step, k, peer, slot):
        return pltpu.make_async_remote_copy(
            src_ref=mine.at[step], dst_ref=sums.at[step, slot],
            send_sem=sum_send.at[step, k], recv_sem=sum_recv.at[step, k],
            device_id=(peer // cols, lax.rem(peer, cols)), device_id_type=MESH,
        )

    def begin_products(step):
        def add(i, carry):
            norm, curve = carry
            here = pl.ds(pl.multiple_of(PAD + i * 32, 8), 32)
            a, c = res[here, 0:width], image[here, 0:width]
            aa, ac = a * a, a * c
            norm = norm + ((aa[:8] + aa[8:16]) + (aa[16:24] + aa[24:]))
            return norm, curve + ((ac[:8] + ac[8:16]) + (ac[16:24] + ac[24:]))

        zero = jnp.zeros((8, width), jnp.float32)
        norm, curve = lax.fori_loop(0, height // 32, add, (zero, zero))
        norm = jnp.sum(jnp.sum(norm, axis=0, keepdims=True), axis=1, keepdims=True)
        curve = jnp.sum(jnp.sum(curve, axis=0, keepdims=True), axis=1, keepdims=True)
        both = jnp.where(lane == 0, norm, jnp.where(lane == 1, curve, 0.0))
        mine[step] = both
        sums[step, me] = both

        def begin(k, carry):
            copy_to(step, k, lax.rem(me + k, count), me).start()
            return carry

        lax.fori_loop(1, count, begin, 0, unroll=True)

    def end_products(step):
        def finish(k, carry):
            source = lax.rem(me + count - k, count)
            copy_to(step, k, source, source).wait()
            return carry

        lax.fori_loop(1, count, finish, 0, unroll=True)
        total = jnp.sum(sums[step], axis=0)
        norm = jnp.sum(jnp.where(lane == 0, total, 0.0), axis=1, keepdims=True)
        curve = jnp.sum(jnp.where(lane == 1, total, 0.0), axis=1, keepdims=True)
        return norm, curve

    operate(res, image)
    begin_products(0)
    norm_now = alpha = None
    for step in range(ITERS):
        if step + 1 < ITERS:
            operate(image, second)
        norm_next, curvature = end_products(step)
        if step == 0:
            ratio = None
            alpha = norm_next / curvature
        else:
            ratio = norm_next / norm_now
            alpha = norm_next / (curvature - ratio * norm_next / alpha)
        norm_now = norm_next

        if step + 1 < ITERS:

            def recede(i, carry, step=step, ratio=ratio, alpha=alpha):
                here = pl.ds(pl.multiple_of(HALO + i * 48, 8), 48)
                way, path, next_path = res[here, :], image[here, :], second[here, :]
                old, old_image = way, path
                if step > 0:
                    way = way + ratio * course[here, :]
                    path = path + ratio * along[here, :]
                    next_path = next_path + ratio * further[here, :]
                course[here, :] = way
                along[here, :] = path
                further[here, :] = next_path
                res[here, :] = old - alpha * path
                image[here, :] = old_image - alpha * next_path
                return carry

            lax.fori_loop(0, (height + 2 * HALO) // 48, recede, 0)
            begin_products(step + 1)

        def advance(i, carry, step=step, ratio=ratio, alpha=alpha):
            at = pl.multiple_of(i * 32, 32)
            here = pl.ds(pl.multiple_of(PAD + at, 8), 32)
            rows_here = pl.ds(at, 32)
            if step + 1 < ITERS:
                moved = alpha * course[here, 0:width]
            else:
                moved = alpha * (res[here, 0:width] + ratio * course[here, 0:width])
                r_ref[rows_here, :] = res[here, 0:width] - alpha * (
                    image[here, 0:width] + ratio * along[here, 0:width]
                )
            x_ref[rows_here, :] = moved if step == 0 else x_ref[rows_here, :] + moved
            return carry

        lax.fori_loop(0, height // 32, advance, 0)


def cuts_of(count):
    cuts = list(range(0, count, GROUP)) + [count]
    return cuts[:-1] + [count - GROUP // 2, count]


def edge_and_inner(down, across):
    edge = 2 * across + 2 * (down - 2)
    return edge, (down - 2) * (across - 2)


def edge_tile(e, down, across):
    side = e - across
    last = across + 2 * (down - 2)
    row = jnp.where(e < across, 0, jnp.where(e < last, 1 + side // 2, down - 1))
    col = jnp.where(e < across, e, jnp.where(e < last, lax.rem(side, 2) * (across - 1), e - last))
    return row, col


def inner_tile(e, down, across):
    return 1 + e // (across - 2), 1 + lax.rem(e, across - 2)


def split(value, size):
    if size & (size - 1) == 0:
        return lax.shift_right_logical(value, size.bit_length() - 1), value & (size - 1)
    return lax.div(value, size), lax.rem(value, size)


def digit_steps(place, size):
    return [(1 << n) * (1 - 2 * lax.rem(place // (1 << n), 2)) for n in range(size.bit_length() - 1)]


def flip(place, steps, code):
    for n, step in enumerate(steps):
        if code >> n & 1:
            place = place + step
    return place


def field_kernel(
    rows, cols, cell_hbm, value_hbm, weight_hbm, count_hbm, kappa_hbm,
    fields, coef,
    cell_in, value_in, weight_in, count_in, cell_wide, value_wide, weight_wide,
    code_out, pair_out, code_in, pair_in,
    place_row, place_col, amounts, kap, mid,
    low_out, high_out, low_in, high_in, kap_low_out, kap_high_out, kap_low_in, kap_high_in,
    mine, sums,
    load_sems, send_sem, recv_sems, halo_send, halo_recv, sum_sems,
):
    bw, first, second, third = fields.at[0:2], fields.at[2], fields.at[3], fields.at[4]
    count = rows * cols
    my_row, my_col = lax.axis_index("row"), lax.axis_index("col")
    me = my_row * cols + my_col
    height, width = kappa_hbm.shape
    down, across = height // TILE, width // TILE
    tiles = down * across
    slots = code_in.shape[2]
    edges, inners = edge_and_inner(down, across)
    pitch = cell_wide.shape[0] // tiles
    bottom = MARGIN + height
    lane = lax.broadcasted_iota(jnp.int32, (1, LANES), 1)

    loads = [
        pltpu.make_async_copy(cell_hbm, cell_in, load_sems.at[0]),
        pltpu.make_async_copy(value_hbm, value_in, load_sems.at[1]),
        pltpu.make_async_copy(weight_hbm, weight_in, load_sems.at[2]),
        pltpu.make_async_copy(count_hbm, count_in, load_sems.at[3]),
    ]
    kappa_loads = [
        pltpu.make_async_copy(
            kappa_hbm.at[:, pl.ds(c * LANES, LANES)], kap.at[c, pl.ds(MARGIN, height), :], load_sems.at[4 + c]
        )
        for c in range(across)
    ]
    for load in loads + kappa_loads:
        load.start()

    for ref in (low_in, high_in, kap_low_in, kap_high_in):
        ref[...] = jnp.zeros_like(ref)
    strip = jnp.zeros((MARGIN, LANES), jnp.float32)
    for c in range(across):
        for field in (bw.at[0], bw.at[1], kap):
            field[c, 0:MARGIN, :] = strip
            field[c, bottom : bottom + MARGIN, :] = strip

    row_steps, col_steps = digit_steps(my_row, rows), digit_steps(my_col, cols)
    col_codes = list(range(cols))

    def person(k):
        return flip(my_row, row_steps, k % rows), flip(my_col, col_steps, col_codes[k // rows])

    barrier = pltpu.get_barrier_semaphore()
    with jax.named_scope("greet"):
        for k in reversed(range(1, count)):
            pl.semaphore_signal(barrier, inc=1, device_id=person(k), device_id_type=MESH)

    for field in (bw.at[0], bw.at[1], kap):
        field[across, 0:MARGIN, :] = strip
        field[across, bottom : bottom + MARGIN, :] = strip
    for c in range(across + 1):
        for field in (mid, first, second):
            field[c, 0:8, :] = strip[:8]
            field[c, bottom + 8 : bottom + 16, :] = strip[:8]


    with jax.named_scope("loads"):
        for load in loads:
            load.wait()

    def widen(t, carry):
        here = pl.ds(pl.multiple_of(t * count, 8), count)
        there = pl.ds(pl.multiple_of(t * pitch, 8), count)
        cell_wide[there, :] = cell_in[here, :]
        weight = weight_in[here, :].astype(jnp.float32)
        weight_wide[there, :] = weight
        value_wide[there, :] = weight * value_in[here, :].astype(jnp.float32)
        return carry

    with jax.named_scope("widen"):
        lax.fori_loop(0, tiles, widen, 0)
    dest_lane = lax.broadcasted_iota(jnp.int32, count_in.shape, 1)
    counts = count_in[...].astype(jnp.float32)
    slot_lane = lax.broadcasted_iota(jnp.int32, (tiles, slots), 1).astype(jnp.float32)
    def encode(k):
        row, col = person(k)
        dest = row * cols + col
        every = pl.ds(dest, tiles, stride=pitch)
        cell = cell_wide[every, :]
        upper, _ = split(cell, width * cols)
        line = split(upper, TILE)[1]
        side, place = split(line, FOLD)
        local = place * SPAN + side * TILE + split(cell, TILE)[1]
        alive = jnp.sum(jnp.where(dest_lane == dest, counts, 0.0), axis=1, keepdims=True)
        local = jnp.where(slot_lane < alive, local, -1)
        weight, product = weight_wide[every, :], value_wide[every, :]
        code_out[k] = local.astype(jnp.int16)
        pair_out[k] = jnp.concatenate([weight, product], axis=0).astype(jnp.bfloat16)

    with jax.named_scope("encode"):
        for k in reversed(range(count)):
            encode(k)
    buffers = ((code_out, code_in), (pair_out, pair_in))
    for source, target in buffers:
        target[0] = source[0]
    with jax.named_scope("arrive"):
        await_all(count)

    cuts = cuts_of(count)
    chunks = len(cuts) - 1

    with jax.named_scope("send"):
        for k in range(1, count):
            place = person(k)
            for which, (source, target) in enumerate(buffers):
                pltpu.make_async_remote_copy(
                    src_ref=source.at[k], dst_ref=target.at[k],
                    send_sem=send_sem.at[which], recv_sem=recv_sems.at[sum(k >= cut for cut in cuts[1:]), which],
                    device_id=place, device_id_type=MESH,
                ).start()

    def halo_copies(group, body, parts):
        low_from, high_from, low_to, high_to = parts
        up_rows, down_rows = pl.ds(MARGIN, 8), pl.ds(bottom - 8, 8)
        above, below = pl.ds(MARGIN - 8, 8), pl.ds(bottom, 8)
        main = pl.ds(LANES, height)
        head, tail = pl.ds(0, LANES), pl.ds(LANES + height, LANES)
        begin, end = pl.ds(0, LANES), pl.ds(height - LANES, LANES)
        whole = pl.ds(0, height)
        plan = [
            (-1, 0, body(up_rows), body(below)),
            (1, 0, body(down_rows), body(above)),
            (0, -1, low_from.at[:, whole], high_to.at[:, main]),
            (0, 1, high_from.at[:, whole], low_to.at[:, main]),
            (-1, -1, low_from.at[:, begin], high_to.at[:, tail]),
            (1, -1, low_from.at[:, end], high_to.at[:, head]),
            (-1, 1, high_from.at[:, begin], low_to.at[:, tail]),
            (1, 1, high_from.at[:, end], low_to.at[:, head]),
        ]
        made = []
        for at, (dr, dc, source, target) in enumerate(plan):

            def there(dr=dr, dc=dc):
                ok = True
                for step, place, size in ((dr, my_row, rows), (dc, my_col, cols)):
                    if step < 0:
                        ok = (place > 0) & ok
                    if step > 0:
                        ok = (place < size - 1) & ok
                return ok

            copy = pltpu.make_async_remote_copy(
                src_ref=source, dst_ref=target,
                send_sem=halo_send.at[group, at], recv_sem=halo_recv.at[group, at],
                device_id=(my_row + dr, my_col + dc), device_id_type=MESH,
            )
            made.append((there(), there(-dr, -dc), copy))
        return made

    def start_halo(copies):
        for goes, _, copy in copies:

            @pl.when(goes)
            def _(copy=copy):
                copy.start()

    def end_halo(copies):
        for goes, comes, copy in copies:

            @pl.when(goes)
            def _(copy=copy):
                copy.wait_send()

            @pl.when(comes)
            def _(copy=copy):
                copy.wait_recv()

    def pack(field, at, low, high):
        for j in range(down):
            here = pl.ds(MARGIN + j * TILE, TILE)
            there = slice(j * TILE, (j + 1) * TILE)
            sides = jnp.where(lane < LANES // 2, field[0, here, :], field[across - 1, here, :]).T
            low[at : at + 8, there] = sides[:8]
            high[at : at + 8, there] = sides[TILE - 8 :]

    gap = jnp.zeros((LANES - 16, LANES), jnp.float32)

    def unpack(field, at, low, high):
        for j in range(-1, down + 1):
            lanes = slice(LANES + j * TILE, LANES + (j + 1) * TILE)
            both = jnp.concatenate([high[at : at + 8, lanes], gap, low[at : at + 8, lanes]], axis=0).T
            if j < 0:
                field[across, MARGIN - 8 : MARGIN, :] = both[TILE - 8 :]
            elif j == down:
                field[across, bottom : bottom + 8, :] = both[:8]
            else:
                field[across, MARGIN + j * TILE : MARGIN + (j + 1) * TILE, :] = both

    kap_halo = halo_copies(
        0, lambda part: kap.at[pl.ds(0, across), part, :], (kap_low_out, kap_high_out, kap_low_in, kap_high_in)
    )
    bw_halo = halo_copies(
        1, lambda part: bw.at[:, pl.ds(0, across), part, :], (low_out, high_out, low_in, high_in)
    )
    with jax.named_scope("kappa"):
        for load in kappa_loads:
            load.wait()
        pack(kap, 0, kap_low_out, kap_high_out)
        start_halo(kap_halo)

    offsets = lax.broadcasted_iota(jnp.int32, (SPAN, slots), 0).astype(jnp.float32).astype(jnp.bfloat16)
    one = jnp.ones((SPAN, slots), jnp.bfloat16)
    zero = jnp.zeros((SPAN, slots), jnp.bfloat16)

    def take_chunk(chunk):
        begin, end = max(cuts[chunk], 1), cuts[chunk + 1]
        with jax.named_scope("wait"):
            for which, (_, target) in enumerate(buffers):
                part = target.at[pl.ds(begin, end - begin)]
                pltpu.make_async_copy(part, part, recv_sems.at[chunk, which]).wait()
        with jax.named_scope("spread"):
            for n in range(cuts[chunk], end):
                code = code_in[n].astype(jnp.int32)
                place_row[n * tiles : (n + 1) * tiles, :] = (code >> (SPAN.bit_length() - 1)).astype(jnp.float32)
                place_col[n * tiles : (n + 1) * tiles, :] = (code & (SPAN - 1)).astype(jnp.float32)
                amounts[n * 2 * tiles : (n + 1) * 2 * tiles, :] = pair_in[n].astype(jnp.float32)

    def bin_chunk(begin, end, some, locate):
        def spread(ref, at, size):
            return jnp.broadcast_to(ref[pl.ds(at, 1), :].astype(jnp.bfloat16), (size, slots))

        def bin_tile(e, carry):
            hot, weights, products = [], [], []
            row, col = locate(e, down, across)
            tile = row * across + col
            for n in range(begin, end):
                hit = spread(place_col, n * tiles + tile, SPAN) == offsets
                hot.append(jnp.where(hit, one, zero).astype(jnp.float8_e4m3fn))
                hit = spread(place_row, n * tiles + tile, FOLD) == offsets[:FOLD]
                weights.append(jnp.where(hit, spread(amounts, n * 2 * tiles + tile, FOLD), zero[:FOLD]))
                products.append(jnp.where(hit, spread(amounts, (n * 2 + 1) * tiles + tile, FOLD), zero[:FOLD]))
            stacked = jnp.concatenate(
                [jnp.concatenate(products, axis=1), jnp.concatenate(weights, axis=1)], axis=0
            )
            total = lax.dot_general(
                stacked, jnp.concatenate(hot, axis=1), (((1,), (1,)), ((), ())),
                preferred_element_type=jnp.float32,
            )
            for n in range(TILE // FOLD):
                here = pl.ds(pl.multiple_of(MARGIN + row * TILE + n * FOLD, 8), FOLD)
                lanes = slice(n * TILE, (n + 1) * TILE)
                for which in range(2):
                    part = total[which * FOLD : (which + 1) * FOLD, lanes]
                    if begin == 0:
                        bw[which, col, here, :] = part
                    else:
                        bw[which, col, here, :] += part
            return carry

        with jax.named_scope("bin"):
            lax.fori_loop(0, some, bin_tile, 0, unroll=TILES_AT_ONCE)

    for chunk in range(chunks):
        take_chunk(chunk)
        bin_chunk(cuts[chunk], cuts[chunk + 1], edges, edge_tile)
    with jax.named_scope("pack"):
        for which in range(2):
            pack(bw.at[which], 8 * which, low_out, high_out)
        start_halo(bw_halo)
    for begin in range(0, count, GROUP):
        bin_chunk(begin, begin + GROUP, inners, inner_tile)
    with jax.named_scope("kap_halo"):
        end_halo(kap_halo)
        unpack(kap, 0, kap_low_in, kap_high_in)

        def lift(i, carry):
            here = pl.ds(pl.multiple_of(i * 16, 8), 16)
            for c in range(across + 1):
                kap[c, here, :] = 4.0 + kap[c, here, :]
            return carry

        lax.fori_loop(0, kap.shape[1] // 16, lift, 0, unroll=2)
    with jax.named_scope("sent"):
        for which, (source, _) in enumerate(buffers):
            part = source.at[pl.ds(1, count - 1)]
            pltpu.make_async_copy(part, part, send_sem.at[which]).wait()
    with jax.named_scope("halo"):
        end_halo(bw_halo)
    with jax.named_scope("unpack"):
        for which in range(2):
            unpack(bw.at[which], 8 * which, low_in, high_in)

    up, under = my_row > 0, my_row < rows - 1
    live = ((lane < 8) & (my_col < cols - 1)) | ((lane >= LANES - 8) & (my_col > 0))

    def inner(field, at, size, columns):
        every = range(across + 1)
        here = pl.ds(at, size)
        center = [field[c, here, :] for c in every]
        ahead = [pltpu.roll(x, 1, axis=1) for x in center]
        behind = [pltpu.roll(x, LANES - 1, axis=1) for x in center]
        result = []
        for c in range(columns):
            beside = field[c, pl.ds(at - 1, size), :] + field[c, pl.ds(at + 1, size), :]
            beside = beside + jnp.where(lane == 0, ahead[c - 1], ahead[c])
            beside = beside + jnp.where(lane == LANES - 1, behind[(c + 1) % (across + 1)], behind[c])
            value = kap[c, here, :] * center[c] - beside
            result.append(jnp.where(live, value, 0.0) if c == across else value)
        return result

    response, weight = bw.at[0], bw.at[1]
    outer = ((MARGIN - 8, up), (bottom, under))

    def bands(body, carry):
        def step(i, carry):
            return body(pl.multiple_of(MARGIN + i * BAND, 8), carry)

        return lax.fori_loop(0, height // BAND, step, carry, unroll=UNROLL)

    def fold(value):
        total = value[0:8]
        for n in range(8, value.shape[0], 8):
            total = total + value[n : n + 8]
        return total

    blank = jnp.zeros((8, LANES), jnp.float32)

    def apply_inner(source, measure=False):
        def body(at, carry):
            for c, value in enumerate(inner(source, at, BAND, across + 1)):
                here = pl.ds(at, BAND)
                mid[c, here, :] = value
                if measure and c < across:
                    square, energy = carry
                    x = source[c, here, :]
                    xx = x * x
                    square = square + fold(xx)
                    energy = energy + fold(weight[c, here, :] * xx + smooth_weight * (value * value))
                    carry = square, energy
            return carry

        result = bands(body, (blank, blank) if measure else 0)
        for at, there in outer:
            for c, value in enumerate(inner(source, at, 8, across + 1)):
                mid[c, pl.ds(at, 8), :] = jnp.where(there, value, 0.0)
        return result

    def apply_outer(source, target):
        def body(at, carry):
            square, energy = carry
            for c, value in enumerate(inner(mid, at, BAND, across + 1)):
                here = pl.ds(at, BAND)
                x = source[c, here, :]
                value = weight[c, here, :] * x + smooth_weight * value
                target[c, here, :] = value
                if c < across:
                    square = square + fold(x * x)
                    energy = energy + fold(x * value)
            return square, energy

        result = bands(body, (blank, blank))
        for at, there in outer:
            for c, value in enumerate(inner(mid, at, 8, across + 1)):
                here = pl.ds(at, 8)
                value = weight[c, here, :] * source[c, here, :] + smooth_weight * value
                target[c, here, :] = jnp.where(there, value, 0.0)
        return result

    moments = []
    with jax.named_scope("op1"):
        apply_inner(response)
    with jax.named_scope("op2"):
        moments += apply_outer(response, first)
    with jax.named_scope("op3"):
        apply_inner(first)
    with jax.named_scope("op4"):
        moments += apply_outer(first, second)
    with jax.named_scope("op5"):
        moments += apply_inner(second, True)

    with jax.named_scope("fold"):
        both = jnp.zeros((1, LANES), jnp.float32)
        for at, value in enumerate(moments):
            total = jnp.sum(jnp.sum(value, axis=0, keepdims=True), axis=1, keepdims=True)
            both = jnp.where(lane == at, total, both)
        mine[...] = both
        sums[me] = both

    with jax.named_scope("sum_send"):
        for k in reversed(range(1, count)):
            pltpu.make_async_remote_copy(
                src_ref=mine, dst_ref=sums.at[me],
                send_sem=sum_sems.at[0], recv_sem=sum_sems.at[1],
                device_id=person(k), device_id_type=MESH,
            ).start()

    def last(at, carry):
        for c, value in enumerate(inner(mid, at, BAND, across)):
            here = pl.ds(at, BAND)
            third[c, here, :] = weight[c, here, :] * second[c, here, :] + smooth_weight * value
        return carry

    with jax.named_scope("op6"):
        bands(last, 0)

    with jax.named_scope("sum_wait"):
        part = sums.at[pl.ds(1, count - 1)]
        for n in range(2):
            pltpu.make_async_copy(part, part, sum_sems.at[n]).wait()
    coef_scope = jax.named_scope("coef")
    coef_scope.__enter__()
    total = [sums[n] for n in range(count)]
    while len(total) > 1:
        total = [total[n] + total[n + 1] for n in range(0, len(total), 2)]
    total = total[0]
    m = [jnp.sum(jnp.where(lane == at, total, 0.0), axis=1, keepdims=True) for at in range(6)]
    scale = m[1] / m[0]
    power, n = scale, [None, None]
    for at in range(2, 6):
        power = power * scale
        n.append(m[at] / m[0] / power)
    fall = n[2] - 1.0
    bend = n[3] - n[2] * n[2]
    alpha = fall / bend
    a = 1.0 + alpha * n[2]
    lead = n[2] - a * n[3] + alpha * n[4]
    lead_size = n[2] + a * n[3] + alpha * n[4]
    beta = alpha * lead / fall
    d0, d1 = 1.0 + beta * n[2], a + beta
    turn = d0 * n[3] - d1 * n[4] + alpha * n[5]
    turn_size = d0 * n[3] + d1 * n[4] + alpha * n[5]
    step = lead / turn
    inverse = 1.0 / scale
    powers = [inverse, inverse * inverse, inverse * inverse * inverse]
    parts = [
        (1.0 + alpha * n[2] + step * d0) * powers[0],
        -(alpha + step * d1) * powers[1],
        step * alpha * powers[2],
        -(a + step * d0) * powers[0],
        (alpha + step * d1) * powers[1],
        -(step * alpha) * powers[2],
    ]
    for at, value in enumerate(parts):
        coef[at : at + 1, :] = jnp.broadcast_to(value, (1, LANES))
    sound = (fall * LIMIT >= n[2]) & (bend * LIMIT >= n[3])
    sound = sound & (lead * LIMIT >= lead_size) & (turn * LIMIT >= turn_size)
    sound = sound & (alpha * lead * (2.0 * LIMIT) >= 1.0 + a * a * n[2] + alpha * alpha * n[4])
    coef[6:8, :] = jnp.broadcast_to(jnp.where(sound, 1.0, 0.0), (2, LANES))
    coef_scope.__exit__(None, None, None)


def combine_kernel(fields, coef, x_hbm, r_hbm, x_out, r_out, sems):
    height, width = x_hbm.shape
    across = width // LANES
    band = height // 8
    weights = [coef[at : at + 1, :] for at in range(6)]
    copies = []
    for i in range(8):
        rows_here = pl.ds(i * band, band)

        def body(j, carry, i=i):
            at = pl.multiple_of(i * band + j * 32, 8)
            for c in range(across):
                here = pl.ds(MARGIN + at, 32)
                values = [fields[n, c, here, :] for n in (0, 2, 3, 4)]
                lanes = slice(c * LANES, (c + 1) * LANES)
                x_out[pl.ds(at, 32), lanes] = (
                    weights[0] * values[0] + weights[1] * values[1] + weights[2] * values[2]
                )
                r_out[pl.ds(at, 32), lanes] = (
                    values[0] + weights[3] * values[1] + weights[4] * values[2] + weights[5] * values[3]
                )
            return carry

        lax.fori_loop(0, band // 32, body, 0)
        for at, (source, target) in enumerate(((x_out, x_hbm), (r_out, r_hbm))):
            copy = pltpu.make_async_copy(source.at[rows_here], target.at[rows_here], sems.at[i, at])
            copy.start()
            copies.append(copy)
    for copy in copies:
        copy.wait()


def copy_kernel(x_in, r_in, x_out, r_out):
    x_out[...] = x_in[...]
    r_out[...] = r_in[...]


def per_device(rows, cols, obs_cell, obs_value, obs_weight, obs_count, kappa_field):
    count = rows * cols
    height, width = kappa_field.shape
    tiles, _, slots = obs_cell.shape[1:]
    down, across = height // TILE, width // TILE
    in_vmem = pl.BlockSpec(memory_space=pltpu.VMEM)
    in_hbm = pl.BlockSpec(memory_space=pltpu.HBM)
    tall = height + 2 * MARGIN
    field = jax.ShapeDtypeStruct((height, width), jnp.float32)
    wide = jax.ShapeDtypeStruct((across + 1, tall, LANES), jnp.float32)
    pitch = count + 8
    flat = (tiles * count, slots)
    pitched = (tiles * pitch, slots)
    blocks = [
        pltpu.VMEM((count, tiles, slots), jnp.int16),
        pltpu.VMEM((count, 2 * tiles, slots), jnp.bfloat16),
    ]
    fields, coef = pl.pallas_call(
        functools.partial(field_kernel, rows, cols),
        out_shape=(
            jax.ShapeDtypeStruct((5, across + 1, tall, LANES), jnp.float32),
            jax.ShapeDtypeStruct((8, LANES), jnp.float32),
        ),
        in_specs=[in_hbm] * 5,
        out_specs=(in_vmem,) * 2,
        scratch_shapes=[
            pltpu.VMEM(flat, jnp.int32),
            pltpu.VMEM(flat, jnp.bfloat16),
            pltpu.VMEM(flat, jnp.bfloat16),
            pltpu.VMEM((tiles, count), jnp.int32),
            pltpu.VMEM(pitched, jnp.int32),
            pltpu.VMEM(pitched, jnp.float32),
            pltpu.VMEM(pitched, jnp.float32),
            *blocks,
            *blocks,
            pltpu.VMEM(flat, jnp.float32),
            pltpu.VMEM(flat, jnp.float32),
            pltpu.VMEM((2 * tiles * count, slots), jnp.float32),
            pltpu.VMEM(wide.shape, jnp.float32),
            pltpu.VMEM(wide.shape, jnp.float32),
            pltpu.VMEM((16, height), jnp.float32),
            pltpu.VMEM((16, height), jnp.float32),
            pltpu.VMEM((16, height + 2 * LANES), jnp.float32),
            pltpu.VMEM((16, height + 2 * LANES), jnp.float32),
            pltpu.VMEM((8, height), jnp.float32),
            pltpu.VMEM((8, height), jnp.float32),
            pltpu.VMEM((8, height + 2 * LANES), jnp.float32),
            pltpu.VMEM((8, height + 2 * LANES), jnp.float32),
            pltpu.VMEM((1, LANES), jnp.float32),
            pltpu.VMEM((count, 1, LANES), jnp.float32),
            pltpu.SemaphoreType.DMA((4 + across,)),
            pltpu.SemaphoreType.DMA((2,)),
            pltpu.SemaphoreType.DMA((len(cuts_of(count)) - 1, 2)),
            pltpu.SemaphoreType.DMA((2, 8)),
            pltpu.SemaphoreType.DMA((2, 8)),
            pltpu.SemaphoreType.DMA((2,)),
        ],
        compiler_params=pltpu.CompilerParams(
            collective_id=0, has_side_effects=True, vmem_limit_bytes=ROOM
        ),
        name="fields",
    )(
        obs_cell.reshape(flat), obs_value.reshape(flat), obs_weight.reshape(flat),
        obs_count[0], kappa_field,
    )

    def combine(fields, coef, *unused):
        return pl.pallas_call(
            combine_kernel,
            out_shape=(field, field),
            in_specs=[in_vmem] * 2,
            out_specs=(in_hbm,) * 2,
            scratch_shapes=[
                pltpu.VMEM(field.shape, jnp.float32),
                pltpu.VMEM(field.shape, jnp.float32),
                pltpu.SemaphoreType.DMA((8, 2)),
            ],
            compiler_params=pltpu.CompilerParams(vmem_limit_bytes=16 << 20),
            name="combine",
        )(fields, coef)

    def iterate(fields, coef, kappa):
        own = fields[:2, :across, MARGIN : MARGIN + height, :].transpose(0, 2, 1, 3).reshape(2, height, width)
        return pl.pallas_call(
            copy_kernel,
            out_shape=(field, field),
            in_specs=[in_vmem] * 2,
            out_specs=(in_vmem,) * 2,
            name="hand_on",
        )(*smooth(rows, cols, own[0], own[1], kappa))

    return lax.cond(coef[6, 0] > 0, combine, iterate, fields, coef, kappa_field)


def smooth(rows, cols, response, weight_field, kappa_field):
    count = rows * cols
    height, width = kappa_field.shape
    in_vmem = pl.BlockSpec(memory_space=pltpu.VMEM)
    field = jax.ShapeDtypeStruct((height, width), jnp.float32)
    full = width + 128
    tall = -(-(height + 2 * PAD) // 128) * 128
    extended = pltpu.VMEM((tall, full), jnp.float32)
    edge = pltpu.VMEM((3 * HALO, tall), jnp.float32)
    return pl.pallas_call(
        functools.partial(smooth_kernel, rows, cols),
        out_shape=(field, field),
        in_specs=[in_vmem] * 3,
        out_specs=(in_vmem,) * 2,
        scratch_shapes=[extended] * 10
        + [edge] * 4
        + [
            pltpu.VMEM((ITERS, 1, 128), jnp.float32),
            pltpu.VMEM((ITERS, count, 1, 128), jnp.float32),
            pltpu.SemaphoreType.DMA((2, 3)),
            pltpu.SemaphoreType.DMA((2, 3)),
            pltpu.SemaphoreType.DMA((2,)),
            pltpu.SemaphoreType.DMA((2,)),
            pltpu.SemaphoreType.DMA((ITERS, count)),
            pltpu.SemaphoreType.DMA((ITERS, count)),
        ],
        compiler_params=pltpu.CompilerParams(collective_id=1, has_side_effects=True, vmem_limit_bytes=32 << 20),
        name="smoothing",
    )(response, weight_field, kappa_field)


def solution(mesh):
    placed = (
        P(("row", "col"), None, None, None),
        P(("row", "col"), None, None, None),
        P(("row", "col"), None, None, None),
        P(("row", "col"), None, None),
        P("row", "col"),
    )
    return jax.shard_map(
        functools.partial(per_device, mesh.shape["row"], mesh.shape["col"]),
        mesh=mesh,
        in_specs=placed,
        out_specs=(P("row", "col"), P("row", "col")),
        check_vma=False,
    )
```
